512 devices in a mesh: grp: 128 (over y, z, core), slab: 4 (over x).
Axes of the slice: x: 4, y: 8, z: 8, core: 2. Of those that a mesh axis runs over, the one named last changes fastest.
Arguments:
- grids: float32 [128, 512, 4096], P('grp', 'slab'), may hold values from -6 to 6
- first_level: int32 [128], P('grp'), may hold values from 6 to 8, as said below
- coeffs: int32 [128], P('grp'), may hold values from -3 to 3
- slot_map: int32 [128, 512], P('grp', 'slab'), may hold values from 0 to 1023, as said below
Outputs:
- combined_grid: float32 [128, 512, 4096], P('grp', 'slab')
The draws below stay inside these ranges and needn't reach their ends.
Inputs may be any that keep to these rules, and one draw needn't show every extreme that they name: The second dimension of grid g has level 9 minus first_level[g]. Every value of the range is taken by some grid. `slot_map`: grid g's point with first coordinate i of 2^a points lies at position i / 2^a of a periodic unit interval, and likewise in the second dimension. Two rows of any grids at the same position in the first two dimensions share a slot; rows of one grid have distinct slots; every slot is used by some grid. The rows held by the s-th index of slab (first coordinates in the s-th of 4 equal ranges) of every grid have slots in the s-th of 4 equal aligned ranges of the 1024 slots.
All inputs are finite; a program needn't handle non-finite values.
Results may differ from the reference program's by a relative error of at most 0.0003.
Values sent between devices are 32-bit elements; how exact they have to be, the bound alone decides.
No kernel may reach another device: no remote copies, remote signals or barrier semaphores. Data moves between devices by JAX's collectives and lax.ppermute only.
A program may use at most 64 MiB of HBM per device.

```python
import jax
import jax.numpy as jnp
from jax import lax

P2 = 16
P3 = 16
P4 = 16
LEVEL_SUM = 9
GROUPS = 128
ROWS = 512
INNER = 4096
N_SLAB = 4


def level_draw(key):
    order = jax.random.permutation(jax.random.fold_in(key, 11), GROUPS)
    return (LEVEL_SUM - 3 + order % 3).astype(jnp.int32)


def draw_first_level(key, part):
    return level_draw(key)


def draw_slot_map(key, part):
    first = level_draw(key)[:, None]
    second = LEVEL_SUM - first
    row_ids = jnp.arange(ROWS, dtype=jnp.int32)[None, :]
    along_first = row_ids >> second
    along_second = row_ids & (1 << second) - 1
    rev_first = jnp.zeros((GROUPS, ROWS), jnp.int32)
    rev_second = jnp.zeros((GROUPS, ROWS), jnp.int32)
    for place in range(LEVEL_SUM):
        up_first = jnp.maximum(first - 1 - place, 0)
        up_second = jnp.maximum(second - 1 - place, 0)
        rev_first = rev_first + jnp.where(place < first, (along_first >> place & 1) << up_first, 0)
        rev_second = rev_second + jnp.where(place < second, (along_second >> place & 1) << up_second, 0)
    slab_of = along_first * N_SLAB >> first
    coarse = rev_first // N_SLAB
    per_slab = 2 * ROWS // N_SLAB
    band_one = ROWS // N_SLAB
    band_two = band_one + ROWS // (2 * N_SLAB)
    rank = jnp.where(rev_second < 2, coarse * 2 + rev_second, jnp.where(rev_second < 4, band_one + coarse * 2 + rev_second - 2, band_two + coarse * 4 + rev_second - 4))
    keys = jax.random.split(jax.random.fold_in(key, 23), N_SLAB)
    shuffles = jax.vmap(lambda single: jax.random.permutation(single, per_slab))(keys)
    return (slab_of * per_slab + shuffles[slab_of, rank]).astype(jnp.int32)


def set_ends(entries, own_key, least, high):
    longest = entries.shape.index(max(entries.shape))
    spots = []
    for shift in (0, 1):
        where = [jax.random.randint(jax.random.fold_in(own_key, axis), (), 0, length) for axis, length in enumerate(entries.shape)]
        where[longest] = (where[longest] + shift) % entries.shape[longest]
        spots.append(tuple(where))
    return entries.at[spots[0]].set(least).at[spots[1]].set(high)


def level_of(stream_key, extent, cuts, smallest, top_value):
    def one(axis_at, parts):
        heights = jax.random.uniform(jax.random.fold_in(jax.random.fold_in(stream_key, 6), axis_at), (parts,), jnp.float32, smallest / len(cuts), top_value / len(cuts))
        return jnp.repeat(jnp.exp(heights), extent[axis_at] // parts).reshape((-1,) + (1,) * (len(extent) - axis_at - 1))

    loudness = one(*cuts[0])
    for cut in cuts[1:]:
        loudness = loudness * one(*cut)
    return loudness


def noise(key, extent, scale, limit, pieces=(), held_as=jnp.bfloat16):
    level = level_of(key, extent, pieces, -0.22, 0.18) if pieces else 1.0
    result = jax.random.normal(key, extent, jnp.float32) * scale * level
    return jnp.minimum(jnp.maximum(result, -limit), limit).astype(held_as)


def setup_inputs(seed: int = 0) -> dict:
    seeds = jax.random.split(jax.random.key(seed), 5)
    grids = noise(seeds[0], (GROUPS, ROWS, INNER), 1.0, 6.0, ((0, 128), (1, 4)), jnp.float32)
    first_level = draw_first_level(jax.random.fold_in(seeds[4], 71), 0)
    coeffs = set_ends(jax.random.randint(seeds[2], (GROUPS,), -3, 4), jax.random.fold_in(seeds[2], 1), -3, 3).astype(jnp.int32)
    slot_map = draw_slot_map(jax.random.fold_in(seeds[4], 71), 0)
    return dict(grids=grids, first_level=first_level, coeffs=coeffs, slot_map=slot_map)


def hier_weight(target, source, period):
    spread = target & (-target)
    interior = (target != 0).astype(jnp.float32)
    left_side = (source == target - spread).astype(jnp.float32)
    right_side = (source == (target + spread) % period).astype(jnp.float32)
    return (target == source).astype(jnp.float32) - 0.5 * interior * (left_side + right_side)


def dehier_weight(target, source, period):
    spread = jnp.maximum(source & (-source), 1).astype(jnp.float32)
    apart = jnp.abs(target - source)
    apart = jnp.minimum(apart, period - apart).astype(jnp.float32)
    return jnp.where(source == 0, 1.0, jnp.maximum(0.0, 1.0 - apart / spread))


def square_table(maker, length):
    points = jnp.arange(length, dtype=jnp.int32)
    return maker(points[:, None], points[None, :], length)


def inner_apply(values, third_op, rest_op):
    count = values.shape[0]
    shaped = values.reshape(count, P2, P3 * P4)
    shaped = jnp.einsum("ij,rjk->rik", third_op, shaped, precision=lax.Precision.HIGHEST)
    shaped = jnp.einsum("rjk,lk->rjl", shaped, rest_op, precision=lax.Precision.HIGHEST)
    return shaped.reshape(count, P2 * P3 * P4)


def row_matrix(maker, level):
    second = LEVEL_SUM - level
    row_ids = jnp.arange(ROWS, dtype=jnp.int32)
    first_pos = row_ids >> second
    second_pos = row_ids & ((1 << second) - 1)
    first_part = maker(first_pos[:, None], first_pos[None, :], 1 << level)
    second_part = maker(second_pos[:, None], second_pos[None, :], 1 << second)
    return first_part * second_part


def reference(grids, first_level, coeffs, slot_map):
    hier_third = square_table(hier_weight, P2)
    hier_rest = jnp.kron(square_table(hier_weight, P3), square_table(hier_weight, P4))
    back_third = square_table(dehier_weight, P2)
    back_rest = jnp.kron(square_table(dehier_weight, P3), square_table(dehier_weight, P4))

    def add_group(table, item):
        grid, level, factor, slots = item
        mixed = jnp.dot(row_matrix(hier_weight, level), grid, precision=lax.Precision.HIGHEST, preferred_element_type=jnp.float32)
        surplus = inner_apply(mixed, hier_third, hier_rest)
        return table.at[slots].add(factor.astype(jnp.float32) * surplus), None

    table, unused = lax.scan(add_group, jnp.zeros((2 * ROWS, P2 * P3 * P4), jnp.float32), (grids, first_level, coeffs, slot_map))

    def rebuild(item):
        level, slots = item
        values = table[slots]
        nodal = jnp.dot(row_matrix(dehier_weight, level), values, precision=lax.Precision.HIGHEST, preferred_element_type=jnp.float32)
        return inner_apply(nodal, back_third, back_rest)

    return lax.map(rebuild, (first_level, slot_map))
```

```python
import functools

import jax
import jax.numpy as jnp
import numpy as np
from jax import lax
from jax.experimental import pallas as pl
from jax.experimental.pallas import tpu as pltpu
from jax.sharding import PartitionSpec as P

LEVEL_SUM = 9
LOW_LEVEL = 6
NY = 8
NZ = 8
MEMBERS = 8
CROSS = 16
ROWS = 128
PLANE = 8
EXT = 144
BACK = 136
PART = 72
BLOCK = 32
LANES = 128
BLOCKS_OF = {6: (0, 1, 3, 4), 7: (0, 1, 2, 5), 8: (0, 2, 6, 7)}


def place_of(x, y):
    if x % 4 == 0 and y % 4 == 0:
        return (x // 4) * 2 + y // 4
    if x % 4 == 0 and y % 2 == 0:
        return 32 + (x // 4) * 2 + y // 4
    if x % 4 == 2 and y % 4 == 0:
        return 64 + (x // 4) * 2 + y // 4
    if x % 4 == 0:
        return 96 + (x // 4) * 4 + y // 2
    if x % 4 == 2:
        return 160 + (x // 4) * 2 + y // 4
    return 192 + (x // 2) * 2 + y // 4


def hier_line(n):
    h = np.zeros((n, n), np.float32)
    for j in range(n):
        h[j, j] += 1.0
        if j:
            s = j & -j
            h[j, j - s] -= 0.5
            h[j, (j + s) % n] -= 0.5
    return h


def dehier_line(n):
    e = np.zeros((n, n), np.float32)
    e[:, 0] = 1.0
    for k in range(1, n):
        for j in range(n):
            d = min(abs(j - k), n - abs(j - k))
            e[j, k] = max(0.0, 1.0 - d / (k & -k))
    return e


@functools.cache
def row_tables():
    forth = np.zeros((3, EXT, EXT), np.float32)
    back = np.zeros((3, ROWS, EXT), np.float32)
    for level in (6, 7, 8):
        n = 1 << (LEVEL_SUM - level)
        span = ROWS // n
        hy, ey = hier_line(n), dehier_line(n)
        blocks = BLOCKS_OF[level]
        f, g = forth[level - LOW_LEVEL], back[level - LOW_LEVEL]
        for i in range(span):
            for y in range(n):
                t = place_of(i * 64 // span, y * 8 // n)
                m = BLOCK * blocks.index(t // BLOCK) + t % BLOCK
                s = i & -i
                steps = [(i, 1.0)] + ([(i - s, -0.5), (i + s, -0.5)] if i else [])
                for j, w in steps:
                    f[m, j * n : j * n + n] += w * hy[y]
                for j in range(span):
                    w = max(0.0, 1.0 - abs(j - i) / s) if i else 1.0 - j / span
                    g[j * n : j * n + n, m] += w * ey[:, y]
        for y in range(n):
            t = ROWS + y * 8 // n
            f[t, ROWS : ROWS + n] += hy[y]
            for j in range(span):
                g[j * n : j * n + n, t] += j / span * ey[:, y]
    return forth, back


def two_part_dot(table, values):
    high = values.astype(jnp.bfloat16)
    low = (values - high.astype(jnp.float32)).astype(jnp.bfloat16)
    dot = functools.partial(jnp.dot, preferred_element_type=jnp.float32)
    return dot(table, high) + dot(table, low)


def forth_kernel(level_ref, table_ref, rows_ref, next_ref, out_ref):
    width = rows_ref.shape[1]
    values = jnp.concatenate(
        [rows_ref[...], next_ref[...], jnp.zeros((EXT - BACK, width), jnp.float32)], axis=0
    )
    out_ref[0] = two_part_dot(table_ref[...], values)
    level = jnp.broadcast_to(level_ref[0], (EXT - BACK, width))
    out_ref[0, BACK:EXT, :] = level.astype(jnp.float32)


def add_kernel(got_ref, out_ref):
    sums = [None] * 8

    def add(block, value):
        sums[block] = value if sums[block] is None else sums[block] + value

    there = None
    for k in range(MEMBERS):
        level = got_ref[k, BACK : BACK + 1, :]
        six, seven, eight = level == 6.0, level == 7.0, level == 8.0
        first, second, third, fourth = (
            got_ref[k, BLOCK * i : BLOCK * (i + 1), :] for i in range(4)
        )
        add(0, first)
        add(1, jnp.where(eight, 0.0, second))
        add(2, jnp.where(eight, second, jnp.where(seven, third, 0.0)))
        add(3, jnp.where(six, third, 0.0))
        add(4, jnp.where(six, fourth, 0.0))
        add(5, jnp.where(seven, fourth, 0.0))
        add(6, jnp.where(eight, third, 0.0))
        add(7, jnp.where(eight, fourth, 0.0))
        part = got_ref[k, ROWS:BACK, :]
        there = part if there is None else there + part
    pad = jnp.zeros((4 * PART - 8 * BLOCK - PLANE, there.shape[1]), jnp.float32)
    table = jnp.concatenate([*sums, there, pad], axis=0)
    for q in range(4):
        out_ref[q] = table[q * PART : (q + 1) * PART]


def total_kernel(got_ref, out_ref):
    total = got_ref[0]
    for k in range(1, CROSS):
        total = total + got_ref[k]
    for k in range(CROSS):
        out_ref[k] = total


def pick_kernel(table_ref, level_ref, out_ref):
    table = jnp.concatenate([table_ref[q] for q in range(4)], axis=0)
    blocks = [table[BLOCK * i : BLOCK * (i + 1)] for i in range(8)]
    for k in range(MEMBERS):
        level = level_ref[k, 0:1, :]
        six, eight = level == 6.0, level == 8.0
        out_ref[k, 0:32, :] = blocks[0]
        out_ref[k, 32:64, :] = jnp.where(eight, blocks[2], blocks[1])
        out_ref[k, 64:96, :] = jnp.where(six, blocks[3], jnp.where(eight, blocks[6], blocks[2]))
        out_ref[k, 96:128, :] = jnp.where(six, blocks[4], jnp.where(eight, blocks[7], blocks[5]))
        out_ref[k, 128:136, :] = table[256:264]


def back_kernel(table_ref, got_ref, out_ref):
    width = got_ref.shape[2]
    values = jnp.concatenate(
        [got_ref[0], jnp.zeros((EXT - BACK, width), jnp.float32)], axis=0
    )
    out_ref[...] = two_part_dot(table_ref[...], values)


def member(y, z, core):
    return (y * NZ + z) * 2 + core


LINES = [[member(y, z, 0) for y in range(NY)] for z in range(NZ)] + [
    [member(y, z, 1) for z in range(NZ)] for y in range(NY)
]
CROSSES = [
    [member(k, z, 0) for z in range(NZ)] + [member(y, k, 1) for y in range(NY)]
    for k in range(MEMBERS)
]


def exchange(values, groups):
    return lax.all_to_all(values, "grp", 0, 0, axis_index_groups=groups, tiled=True)


def f32(*shape):
    return jax.ShapeDtypeStruct(shape, jnp.float32)


def shards(grids, first_level, coeffs, slot_map):
    rows = grids[0]
    width = rows.shape[1]
    chunk = width // MEMBERS
    lanes = chunk // LANES
    slabs = lax.axis_size("slab")
    following = lax.ppermute(
        rows[:PLANE], "slab", [(i, (i - 1) % slabs) for i in range(slabs)]
    )
    forth, back = row_tables()
    which = first_level[0] - LOW_LEVEL
    pick = lambda tables: lax.dynamic_index_in_dim(
        jnp.asarray(tables, jnp.bfloat16), which, 0, keepdims=False
    )
    forth_table = pick(forth) * coeffs[0].astype(jnp.bfloat16)
    back_table = pick(back)
    whole = lambda shape: pl.BlockSpec(shape, lambda *_: (0,) * len(shape))

    sent = pl.pallas_call(
        forth_kernel,
        grid=(MEMBERS,),
        in_specs=[
            pl.BlockSpec(memory_space=pltpu.SMEM),
            whole((EXT, EXT)),
            pl.BlockSpec((ROWS, chunk), lambda k: (0, k)),
            pl.BlockSpec((PLANE, chunk), lambda k: (0, k)),
        ],
        out_specs=pl.BlockSpec((1, EXT, chunk), lambda k: (k, 0, 0)),
        out_shape=f32(MEMBERS, EXT, chunk),
        name="forth",
    )(first_level, forth_table, rows, following)
    got = exchange(sent, LINES)

    parts = pl.pallas_call(
        add_kernel,
        grid=(lanes,),
        in_specs=[pl.BlockSpec((MEMBERS, EXT, LANES), lambda j: (0, 0, j))],
        out_specs=pl.BlockSpec((4, PART, LANES), lambda j: (j, 0, 0)),
        out_shape=f32(CROSS, PART, LANES),
        name="add",
    )(got)
    parts = exchange(parts, CROSSES)

    total = pl.pallas_call(
        total_kernel,
        out_shape=f32(CROSS, PART, LANES),
        name="total",
    )(parts)
    table = exchange(total, CROSSES)

    picked = pl.pallas_call(
        pick_kernel,
        grid=(lanes,),
        in_specs=[
            pl.BlockSpec((4, PART, LANES), lambda j: (j, 0, 0)),
            pl.BlockSpec((MEMBERS, PLANE, LANES), lambda j: (0, BACK // PLANE, 0)),
        ],
        out_specs=pl.BlockSpec((MEMBERS, BACK, LANES), lambda j: (0, 0, j)),
        out_shape=f32(MEMBERS, BACK, chunk),
        name="pick",
    )(table, got)
    final = exchange(picked, LINES)

    out = pl.pallas_call(
        back_kernel,
        grid=(MEMBERS,),
        in_specs=[
            whole((ROWS, EXT)),
            pl.BlockSpec((1, BACK, chunk), lambda k: (k, 0, 0)),
        ],
        out_specs=pl.BlockSpec((ROWS, chunk), lambda k: (0, k)),
        out_shape=f32(ROWS, width),
        name="back",
    )(back_table, final)
    return out[None]


def solution(mesh):
    in_specs = (P("grp", "slab", None), P("grp"), P("grp"), P("grp", "slab"))
    out_specs = P("grp", "slab", None)
    return jax.shard_map(shards, mesh=mesh, in_specs=in_specs, out_specs=out_specs, check_vma=False)
```

```python
import functools

import jax
import jax.numpy as jnp
import numpy as np
from jax import lax
from jax.experimental import pallas as pl
from jax.experimental.pallas import tpu as pltpu
from jax.sharding import PartitionSpec as P

LEVEL_SUM = 9
LOW_LEVEL = 6
NY = 8
NZ = 8
MEMBERS = 8
ROWS = 128
PLANE = 8
BLOCK = 32
SLOTS = 7
THERE = SLOTS * BLOCK
FLAGS = THERE + PLANE
SENT = FLAGS + 8
ENTRY = 2 * (ROWS + PLANE)
PART = 72
LANES = 128
BLOCKS_OF = {6: (0, 1, 3, 4), 7: (0, 1, 2, 5), 8: (0, 2, 6, 7)}


def slots_of(levels):
    six, seven, eight = (level in levels for level in (6, 7, 8))
    third = 3 if six else (5 if seven else None)
    fifth = 6 if eight else (5 if six and seven else None)
    return (0, 1, 2, third, 4, fifth, 7)


def place_of(x, y):
    if x % 4 == 0 and y % 4 == 0:
        return (x // 4) * 2 + y // 4
    if x % 4 == 0 and y % 2 == 0:
        return 32 + (x // 4) * 2 + y // 4
    if x % 4 == 2 and y % 4 == 0:
        return 64 + (x // 4) * 2 + y // 4
    if x % 4 == 0:
        return 96 + (x // 4) * 4 + y // 2
    if x % 4 == 2:
        return 160 + (x // 4) * 2 + y // 4
    return 192 + (x // 2) * 2 + y // 4


def hier_line(n):
    h = np.zeros((n, n), np.float32)
    for j in range(n):
        h[j, j] += 1.0
        if j:
            s = j & -j
            h[j, j - s] -= 0.5
            h[j, (j + s) % n] -= 0.5
    return h


def dehier_line(n):
    e = np.zeros((n, n), np.float32)
    e[:, 0] = 1.0
    for k in range(1, n):
        for j in range(n):
            d = min(abs(j - k), n - abs(j - k))
            e[j, k] = max(0.0, 1.0 - d / (k & -k))
    return e


def one_grid(level, slots):
    n = 1 << (LEVEL_SUM - level)
    span = ROWS // n
    hy, ey = hier_line(n), dehier_line(n)
    forth = np.zeros((SENT, ROWS + PLANE), np.float32)
    back = np.zeros((ROWS, SENT), np.float32)
    for i in range(span):
        for y in range(n):
            t = place_of(i * 64 // span, y * 8 // n)
            m = BLOCK * slots.index(t // BLOCK) + t % BLOCK
            s = i & -i
            steps = [(i, 1.0)] + ([(i - s, -0.5), (i + s, -0.5)] if i else [])
            for j, w in steps:
                forth[m, j * n : j * n + n] += w * hy[y]
            for j in range(span):
                w = max(0.0, 1.0 - abs(j - i) / s) if i else 1.0 - j / span
                back[j * n : j * n + n, m] += w * ey[:, y]
    for y in range(n):
        t = THERE + y * 8 // n
        forth[t, ROWS : ROWS + n] += hy[y]
        for j in range(span):
            back[j * n : j * n + n, t] += j / span * ey[:, y]
    return forth, back


@functools.cache
def row_tables():
    forth, back = [], []
    for own in (6, 7, 8):
        for other in (6, 7, 8):
            slots = slots_of((own, other))
            mine, theirs = one_grid(own, slots), one_grid(other, slots)
            forth.append(np.concatenate([mine[0], theirs[0]], axis=1))
            back.append(mine[1])
    return np.stack(forth), np.stack(back)


def two_part_dot(table, values):
    high = values.astype(jnp.bfloat16)
    low = (values - high.astype(jnp.float32)).astype(jnp.bfloat16)
    dot = functools.partial(jnp.dot, preferred_element_type=jnp.float32)
    return dot(table, high) + dot(table, low)


def number_in(ref, row):
    return jnp.max(ref[row : row + 1, :LANES])


def forth_kernel(core_ref, level_ref, coeff_ref, table_ref, own_ref, own_next_ref, other_ref, other_next_ref, out_ref):
    own_level = level_ref[0]
    other_level = number_in(other_next_ref, PLANE).astype(jnp.int32)
    own_coeff = coeff_ref[0].astype(jnp.float32)
    other_coeff = other_next_ref[PLANE + 1 : PLANE + 2, :]
    which = (own_level - LOW_LEVEL) * 3 + other_level - LOW_LEVEL
    values = jnp.concatenate(
        [
            own_ref[...] * own_coeff,
            own_next_ref[...] * own_coeff,
            other_ref[...] * other_coeff,
            other_next_ref[:PLANE] * other_coeff,
        ],
        axis=0,
    )
    out_ref[0] = two_part_dot(table_ref[which], values)
    six = jnp.logical_or(own_level == 6, other_level == 6).astype(jnp.float32)
    eight = jnp.logical_or(own_level == 8, other_level == 8).astype(jnp.float32)
    line = lax.broadcasted_iota(jnp.int32, (SENT - FLAGS, values.shape[1]), 0)
    out_ref[0, FLAGS:SENT, :] = jnp.where(line == 0, six, eight)


def add_kernel(got_ref, out_ref):
    sums = [None] * 9

    def add(block, value):
        sums[block] = value if sums[block] is None else sums[block] + value

    for k in range(MEMBERS):
        six = got_ref[k, FLAGS : FLAGS + 1, :] == 1.0
        eight = got_ref[k, FLAGS + 1 : FLAGS + 2, :] == 1.0
        slot = [got_ref[k, BLOCK * i : BLOCK * (i + 1), :] for i in range(SLOTS)]
        add(0, slot[0])
        add(1, slot[1])
        add(2, slot[2])
        add(3, jnp.where(six, slot[3], 0.0))
        add(4, slot[4])
        add(5, jnp.where(six, jnp.where(eight, 0.0, slot[5]), slot[3]))
        add(6, jnp.where(eight, slot[5], 0.0))
        add(7, slot[6])
        add(8, got_ref[k, THERE:FLAGS, :])
    pad = jnp.zeros((4 * PART - 8 * BLOCK - PLANE, sums[0].shape[1]), jnp.float32)
    table = jnp.concatenate([*sums, pad], axis=0)
    for q in range(4):
        out_ref[q] = table[q * PART : (q + 1) * PART]


def total_kernel(got_ref, out_ref):
    total = got_ref[0]
    for k in range(1, MEMBERS):
        total = total + got_ref[k]
    for k in range(MEMBERS):
        out_ref[k] = total


def pick_kernel(table_ref, flags_ref, out_ref):
    table = jnp.concatenate([table_ref[q] for q in range(4)], axis=0)
    blocks = [table[BLOCK * i : BLOCK * (i + 1)] for i in range(8)]
    for k in range(MEMBERS):
        six = flags_ref[k, 0:1, :] == 1.0
        eight = flags_ref[k, 1:2, :] == 1.0
        slots = (
            blocks[0],
            blocks[1],
            blocks[2],
            jnp.where(six, blocks[3], blocks[5]),
            blocks[4],
            jnp.where(eight, blocks[6], blocks[5]),
            blocks[7],
        )
        for i, slot in enumerate(slots):
            out_ref[k, BLOCK * i : BLOCK * (i + 1), :] = slot
        out_ref[k, THERE:FLAGS, :] = table[8 * BLOCK : 8 * BLOCK + PLANE]


def back_kernel(core_ref, level_ref, meta_ref, table_ref, got_ref, *rest):
    out_ref = rest[-1]
    other_level = number_in(meta_ref, 0).astype(jnp.int32)
    which = (level_ref[0] - LOW_LEVEL) * 3 + other_level - LOW_LEVEL
    values = jnp.concatenate(
        [got_ref[0], jnp.zeros((SENT - FLAGS, got_ref.shape[2]), jnp.float32)], axis=0
    )
    out_ref[...] = two_part_dot(table_ref[which], values)


def member(y, z, core):
    return (y * NZ + z) * 2 + core


ALONG_Y = [[[member(y, z, core) for y in range(NY)] for z in range(NZ)] for core in (0, 1)]
ALONG_Z = [[[member(y, z, core) for z in range(NZ)] for y in range(NY)] for core in (0, 1)]
FIRST = ALONG_Y[0] + ALONG_Z[1]
SECOND = ALONG_Z[0] + ALONG_Y[1]


def exchange(values, groups):
    return lax.all_to_all(values, "grp", 0, 0, axis_index_groups=groups, tiled=True)


def f32(*shape):
    return jax.ShapeDtypeStruct(shape, jnp.float32)


def shards(grids, first_level, coeffs, slot_map):
    rows = grids[0]
    width = rows.shape[1]
    half = width // 2
    chunk = half // MEMBERS
    lanes = chunk // LANES
    slabs = lax.axis_size("slab")
    members = lax.axis_size("grp")
    core = lax.axis_index("grp") % 2
    swap = [(i, i ^ 1) for i in range(members)]
    mine, theirs = core * half, (1 - core) * half

    def to_previous(values, turn):
        pairs = [
            (g * slabs + s, (g ^ turn) * slabs + (s - 1) % slabs)
            for g in range(members)
            for s in range(slabs)
        ]
        return lax.ppermute(values, ("grp", "slab"), pairs)

    numbers = jnp.concatenate(
        [
            jnp.broadcast_to(first_level.astype(jnp.float32)[:, None], (1, half)),
            jnp.broadcast_to(coeffs.astype(jnp.float32)[:, None], (PLANE - 1, half)),
        ],
        axis=0,
    )
    plane = rows[:PLANE]
    other_next = to_previous(
        jnp.concatenate([lax.dynamic_slice_in_dim(plane, theirs, half, 1), numbers], axis=0), 1
    )
    own_next = to_previous(lax.dynamic_slice_in_dim(plane, mine, half, 1), 0)
    other = lax.ppermute(lax.dynamic_slice_in_dim(rows, theirs, half, 1), "grp", swap)

    forth, back = row_tables()
    forth = jnp.asarray(forth, jnp.bfloat16)
    back = jnp.asarray(back, jnp.bfloat16)
    cores = core.astype(jnp.int32)[None]
    whole = lambda shape: pl.BlockSpec(shape, lambda *_: (0,) * len(shape))
    smem = pl.BlockSpec(memory_space=pltpu.SMEM)

    sent = pl.pallas_call(
        forth_kernel,
        grid_spec=pltpu.PrefetchScalarGridSpec(
            num_scalar_prefetch=1,
            grid=(MEMBERS,),
            in_specs=[
                smem,
                smem,
                whole((9, SENT, ENTRY)),
                pl.BlockSpec((ROWS, chunk), lambda k, c: (0, c[0] * MEMBERS + k)),
                pl.BlockSpec((PLANE, chunk), lambda k, c: (0, k)),
                pl.BlockSpec((ROWS, chunk), lambda k, c: (0, k)),
                pl.BlockSpec((2 * PLANE, chunk), lambda k, c: (0, k)),
            ],
            out_specs=pl.BlockSpec((1, SENT, chunk), lambda k, c: (k, 0, 0)),
        ),
        out_shape=f32(MEMBERS, SENT, chunk),
        name="forth",
    )(cores, first_level, coeffs, forth, rows, own_next, other, other_next)
    got = exchange(sent, FIRST)

    parts = pl.pallas_call(
        add_kernel,
        grid=(lanes,),
        in_specs=[pl.BlockSpec((MEMBERS, SENT, LANES), lambda j: (0, 0, j))],
        out_specs=pl.BlockSpec((4, PART, LANES), lambda j: (j, 0, 0)),
        out_shape=f32(4 * lanes, PART, LANES),
        name="add",
    )(got)
    parts = exchange(parts, SECOND)

    total = pl.pallas_call(
        total_kernel,
        out_shape=f32(MEMBERS, PART, LANES),
        name="total",
    )(parts)
    table = exchange(total, SECOND)

    picked = pl.pallas_call(
        pick_kernel,
        grid=(lanes,),
        in_specs=[
            pl.BlockSpec((4, PART, LANES), lambda j: (j, 0, 0)),
            pl.BlockSpec((MEMBERS, SENT - FLAGS, LANES), lambda j: (0, FLAGS // 8, 0)),
        ],
        out_specs=pl.BlockSpec((MEMBERS, FLAGS, LANES), lambda j: (0, 0, j)),
        out_shape=f32(MEMBERS, FLAGS, chunk),
        name="pick",
    )(table, got)
    final = exchange(picked, FIRST)
    final_other = lax.ppermute(final, "grp", swap)

    def rebuild(values, turn, *filled):
        return pl.pallas_call(
            back_kernel,
            grid_spec=pltpu.PrefetchScalarGridSpec(
                num_scalar_prefetch=1,
                grid=(MEMBERS,),
                in_specs=[
                    smem,
                    pl.BlockSpec((PLANE, LANES), lambda k, c: (1, 0)),
                    whole((9, ROWS, SENT)),
                    pl.BlockSpec((1, FLAGS, chunk), lambda k, c: (k, 0, 0)),
                    *[pl.BlockSpec(memory_space=pl.ANY) for _ in filled],
                ],
                out_specs=pl.BlockSpec(
                    (ROWS, chunk), lambda k, c: (0, (c[0] ^ turn) * MEMBERS + k)
                ),
            ),
            out_shape=f32(ROWS, width),
            input_output_aliases={5: 0} if filled else {},
            cost_estimate=pl.CostEstimate(
                flops=2 * ROWS * SENT * half * 2, bytes_accessed=4 * half * (FLAGS + ROWS), transcendentals=0
            ),
            name="back",
        )(cores, first_level, other_next, back, values, *filled)

    out = rebuild(final_other, 1, rebuild(final, 0))
    return out[None]


def solution(mesh):
    in_specs = (P("grp", "slab", None), P("grp"), P("grp"), P("grp", "slab"))
    out_specs = P("grp", "slab", None)
    return jax.shard_map(shards, mesh=mesh, in_specs=in_specs, out_specs=out_specs, check_vma=False)
```

```python
import functools

import jax
import jax.numpy as jnp
import numpy as np
from jax import lax
from jax.experimental import pallas as pl
from jax.experimental.pallas import tpu as pltpu
from jax.sharding import PartitionSpec as P

LEVEL_SUM = 9
LOW_LEVEL = 6
NY = 8
NZ = 8
MEMBERS = 8
ROWS = 128
BLOCK = 32
SLOTS = 7
EDGE = SLOTS * BLOCK
FLAGS = EDGE + 8
SENT = FLAGS + 8
PART = 64
LANES = 128


def slots_of(levels):
    six, seven, eight = (level in levels for level in (6, 7, 8))
    third = 3 if six else (5 if seven else None)
    fifth = 6 if eight else (5 if six and seven else None)
    return (0, 1, 2, third, 4, fifth, 7)


def place_of(x, y):
    if x % 4 == 0 and y % 4 == 0:
        return (x // 4) * 2 + y // 4
    if x % 4 == 0 and y % 2 == 0:
        return 32 + (x // 4) * 2 + y // 4
    if x % 4 == 2 and y % 4 == 0:
        return 64 + (x // 4) * 2 + y // 4
    if x % 4 == 0:
        return 96 + (x // 4) * 4 + y // 2
    if x % 4 == 2:
        return 160 + (x // 4) * 2 + y // 4
    return 192 + (x // 2) * 2 + y // 4


def hier_line(n):
    h = np.zeros((n, n), np.float32)
    for j in range(n):
        h[j, j] += 1.0
        if j:
            s = j & -j
            h[j, j - s] -= 0.5
            h[j, (j + s) % n] -= 0.5
    return h


def dehier_line(n):
    e = np.zeros((n, n), np.float32)
    e[:, 0] = 1.0
    for k in range(1, n):
        for j in range(n):
            d = min(abs(j - k), n - abs(j - k))
            e[j, k] = max(0.0, 1.0 - d / (k & -k))
    return e


EDGE_ALL = (0, 4, 2, 6, 1, 3, 5, 7)
EDGE_SEVEN = (0, 4, 2, 6)
EDGE_EIGHT = (0, 4)


def one_grid(level, slots):
    n = 1 << (LEVEL_SUM - level)
    span = ROWS // n
    hy, ey = hier_line(n), dehier_line(n)
    forth = np.zeros((SENT, ROWS), np.float32)
    back = np.zeros((ROWS, SENT), np.float32)

    def edge(i, y):
        if i * 64 // span == 63:
            return EDGE + 12 + EDGE_EIGHT.index(y)
        if i * 64 // span == 62:
            return EDGE + 8 + EDGE_SEVEN.index(y)
        return EDGE + EDGE_ALL.index(y)

    for i in range(span):
        for y in range(n):
            up = y * 8 // n
            t = place_of(i * 64 // span, up)
            m = BLOCK * slots.index(t // BLOCK) + t % BLOCK
            s = i & -i
            forth[m, i * n : i * n + n] += hy[y]
            for j in (i - s, i + s) if i else ():
                if j < span:
                    forth[m, j * n : j * n + n] -= 0.5 * hy[y]
            for j in range(span):
                w = max(0.0, 1.0 - abs(j - i) / s) if i else 1.0 - j / span
                back[j * n : j * n + n, m] += w * ey[:, y]
                if i and i + s == span:
                    back[j * n : j * n + n, edge(i, up)] -= 0.5 * w * ey[:, y]
                if i == 0:
                    back[j * n : j * n + n, EDGE + EDGE_ALL.index(up)] += j / span * ey[:, y]
    for y in range(n):
        if level >= 7:
            forth[EDGE + EDGE_SEVEN.index(y * 8 // n), :n] += hy[y]
        if level == 8:
            forth[EDGE + 4 + EDGE_EIGHT.index(y * 8 // n), :n] += hy[y]
    return forth, back


@functools.cache
def row_tables():
    forth, back = [], []
    for own in (6, 7, 8):
        for other in (6, 7, 8):
            slots = slots_of((own, other))
            mine, theirs = one_grid(own, slots), one_grid(other, slots)
            forth.append(np.concatenate([mine[0], theirs[0]], axis=1))
            back.append(mine[1])
    return np.stack(forth), np.stack(back)


def two_part_dot(table, values):
    high = values.astype(jnp.bfloat16)
    low = (values - high.astype(jnp.float32)).astype(jnp.bfloat16)
    dot = functools.partial(jnp.dot, preferred_element_type=jnp.float32)
    return dot(table, high) + dot(table, low)


def number_in(ref, row):
    return jnp.max(ref[row : row + 1, :LANES])


def half_of(ref, core):
    width = ref.shape[1] // 2
    return ref.at[:, pl.ds(pl.multiple_of(core * width, LANES), width)]


def entry_kernel(core_ref, level_ref, coeff_ref, rows_ref, out_ref, sem):
    copy = pltpu.make_async_copy(half_of(rows_ref, 1 - core_ref[0]), out_ref.at[:ROWS], sem)
    copy.start()
    shape = (8, out_ref.shape[1])
    line = lax.broadcasted_iota(jnp.int32, shape, 0)
    out_ref[ROWS:, :] = jnp.where(line == 0, level_ref[0], coeff_ref[0]).astype(jnp.float32)
    copy.wait()


def forth_kernel(core_ref, level_ref, coeff_ref, table_ref, rows_ref, other_ref, out_ref, meta_ref):
    own_level = level_ref[0]
    other_level = number_in(other_ref, ROWS).astype(jnp.int32)
    which = (own_level - LOW_LEVEL) * 3 + other_level - LOW_LEVEL
    chunk = out_ref.shape[2]
    lane = lax.broadcasted_iota(jnp.int32, (1, 2 * ROWS), 1)
    scale = jnp.where(lane < ROWS, coeff_ref[0].astype(jnp.float32), number_in(other_ref, ROWS + 1))
    table = (table_ref[which].astype(jnp.float32) * scale).astype(jnp.bfloat16)
    six = jnp.logical_or(own_level == 6, other_level == 6).astype(jnp.float32)
    eight = jnp.logical_or(own_level == 8, other_level == 8).astype(jnp.float32)
    line = lax.broadcasted_iota(jnp.int32, (SENT - FLAGS, chunk), 0)
    flags = jnp.where(line == 0, six, eight)
    for k in range(MEMBERS):
        start = pl.multiple_of((core_ref[0] * MEMBERS + k) * chunk, LANES)
        own = rows_ref[:, pl.ds(start, chunk)]
        other = other_ref[:ROWS, k * chunk : (k + 1) * chunk]
        values = jnp.concatenate([own, other], axis=0)
        out_ref[k] = two_part_dot(table, values)
        out_ref[k, FLAGS:SENT, :] = flags
    meta_ref[...] = other_ref[ROWS:, :LANES]


def edge_kernel(got_ref, out_ref):
    def total(low, high, held=None):
        total = 0.0
        for k in range(MEMBERS):
            part = got_ref[k, low:high, :]
            total += part if held is None else jnp.where(got_ref[k, held : held + 1, :] == 1.0, part, 0.0)
        return total

    out_ref[0:2, :] = total(0, 8)[0:2]
    out_ref[2:4, :] = total(BLOCK, BLOCK + 8)[0:2]
    out_ref[4:8, :] = total(3 * BLOCK, 3 * BLOCK + 8, FLAGS)[0:4]
    out_ref[8:16, :] = total(EDGE, FLAGS)


def add_kernel(got_ref, out_ref):
    six = [got_ref[k, FLAGS : FLAGS + 1, :] == 1.0 for k in range(MEMBERS)]
    eight = [got_ref[k, FLAGS + 1 : FLAGS + 2, :] == 1.0 for k in range(MEMBERS)]
    slot = lambda k, i: got_ref[k, BLOCK * i : BLOCK * (i + 1), :]
    terms = (
        lambda k: slot(k, 0),
        lambda k: slot(k, 1),
        lambda k: slot(k, 2),
        lambda k: jnp.where(six[k], slot(k, 3), 0.0),
        lambda k: slot(k, 4),
        lambda k: jnp.where(six[k], jnp.where(eight[k], 0.0, slot(k, 5)), slot(k, 3)),
        lambda k: jnp.where(eight[k], slot(k, 5), 0.0),
        lambda k: slot(k, 6),
    )
    for block, term in enumerate(terms):
        total = term(0)
        for k in range(1, MEMBERS):
            total = total + term(k)
        q, low = block // 2, block % 2 * BLOCK
        for j in range(total.shape[1] // LANES):
            out_ref[4 * j + q, low : low + BLOCK, :] = total[:, j * LANES : (j + 1) * LANES]


def total_kernel(got_ref, edge_ref, out_ref):
    total = got_ref[0]
    for k in range(1, MEMBERS):
        total = total + got_ref[k]
    for k in range(MEMBERS):
        out_ref[k, :PART, :] = total
        for j in range(2):
            low = PART + 16 * j
            out_ref[k, low : low + 16, :] = edge_ref[:, j * LANES : (j + 1) * LANES]


def pick_kernel(table_ref, got_ref, out_ref):
    for j in range(2):
        span = slice(j * LANES, (j + 1) * LANES)

        def block(i):
            low = i % 2 * BLOCK
            return table_ref[4 * j + i // 2, low : low + BLOCK, :]

        low = PART + 16 * j
        edge = table_ref[0, low : low + 16, :]
        for k in range(1, MEMBERS):
            edge = edge + table_ref[k, low : low + 16, :]
        for k in range(MEMBERS):
            six = got_ref[k, FLAGS : FLAGS + 1, span] == 1.0
            eight = got_ref[k, FLAGS + 1 : FLAGS + 2, span] == 1.0
            out_ref[k, 0:32, span] = block(0)
            out_ref[k, 32:64, span] = block(1)
            out_ref[k, 64:96, span] = block(2)
            out_ref[k, 96:128, span] = jnp.where(six, block(3), block(5))
            out_ref[k, 128:160, span] = block(4)
            out_ref[k, 160:192, span] = jnp.where(eight, block(6), block(5))
            out_ref[k, 192:224, span] = block(7)
            out_ref[k, EDGE:SENT, span] = edge


def levels_in(level_ref, meta_ref):
    return level_ref[0] - LOW_LEVEL, number_in(meta_ref, 0).astype(jnp.int32) - LOW_LEVEL


def other_back_kernel(level_ref, meta_ref, table_ref, got_ref, out_ref):
    own, other = levels_in(level_ref, meta_ref)
    table = table_ref[other * 3 + own]
    chunk = got_ref.shape[2]
    for k in range(MEMBERS):
        out_ref[:, k * chunk : (k + 1) * chunk] = two_part_dot(table, got_ref[k])


def own_back_kernel(core_ref, level_ref, meta_ref, table_ref, got_ref, out_ref, done_ref, sems):
    own, other = levels_in(level_ref, meta_ref)
    table = table_ref[own * 3 + other]
    chunk = got_ref.shape[2]
    copies = []
    for k in range(MEMBERS):
        done_ref[k] = two_part_dot(table, got_ref[k])
        start = pl.multiple_of((core_ref[0] * MEMBERS + k) * chunk, LANES)
        copy = pltpu.make_async_copy(done_ref.at[k], out_ref.at[:, pl.ds(start, chunk)], sems.at[k])
        copy.start()
        copies.append(copy)
    for copy in copies:
        copy.wait()


def place_kernel(core_ref, values_ref, filled_ref, out_ref, sem):
    copy = pltpu.make_async_copy(values_ref, half_of(out_ref, 1 - core_ref[0]), sem)
    copy.start()
    copy.wait()


def member(y, z, core):
    return (y * NZ + z) * 2 + core


ALONG_Y = [[[member(y, z, core) for y in range(NY)] for z in range(NZ)] for core in (0, 1)]
ALONG_Z = [[[member(y, z, core) for z in range(NZ)] for y in range(NY)] for core in (0, 1)]
FIRST = ALONG_Y[0] + ALONG_Z[1]
SECOND = ALONG_Z[0] + ALONG_Y[1]
VMEM = pl.BlockSpec(memory_space=pltpu.VMEM)
SMEM = pl.BlockSpec(memory_space=pltpu.SMEM)
HBM = pl.BlockSpec(memory_space=pltpu.HBM)
DMA = pltpu.SemaphoreType.DMA


def exchange(values, groups):
    return lax.all_to_all(values, "grp", 0, 0, axis_index_groups=groups, tiled=True)


def f32(*shape):
    return jax.ShapeDtypeStruct(shape, jnp.float32)


def call(kernel, ins, outs, shapes, scratch=(), limit=16, flops=0, moved=0, alias=None):
    return pl.pallas_call(
        kernel,
        in_specs=ins,
        out_specs=outs,
        out_shape=shapes,
        scratch_shapes=scratch,
        compiler_params=pltpu.CompilerParams(vmem_limit_bytes=limit << 20),
        cost_estimate=pl.CostEstimate(flops=flops, bytes_accessed=moved, transcendentals=0),
        input_output_aliases=alias or {},
    )


def shards(grids, first_level, coeffs, slot_map):
    rows = grids[0]
    width = rows.shape[1]
    half = width // 2
    chunk = half // MEMBERS
    slabs = lax.axis_size("slab")
    core = (lax.axis_index("grp") % 2).astype(jnp.int32)[None]
    swap = [(i, i ^ 1) for i in range(lax.axis_size("grp"))]
    to_previous = [(i, (i - 1) % slabs) for i in range(slabs)]
    forth, back = (jnp.asarray(table, jnp.bfloat16) for table in row_tables())

    entry = call(
        entry_kernel, [SMEM, SMEM, SMEM, HBM], VMEM, f32(ROWS + 8, half), (DMA,), limit=60, moved=4 * half * ROWS
    )(core, first_level, coeffs, rows)
    other = lax.ppermute(entry, "grp", swap)
    sent, meta = call(
        forth_kernel, [SMEM, SMEM, SMEM, VMEM, VMEM, VMEM], [VMEM, VMEM],
        [f32(MEMBERS, SENT, chunk), f32(8, LANES)], flops=10**9,
    )(core, first_level, coeffs, forth, rows, other)
    got = exchange(sent, FIRST)

    edge = call(edge_kernel, [VMEM], VMEM, f32(16, chunk), flops=10**6)(got)
    next_edge = lax.ppermute(edge, "slab", to_previous)
    parts = call(add_kernel, [VMEM], VMEM, f32(MEMBERS, PART, LANES), flops=10**8)(got)
    parts = exchange(parts, SECOND)
    total = call(
        total_kernel, [VMEM, VMEM], VMEM, f32(MEMBERS, PART + 32, LANES), flops=10**7
    )(parts, next_edge)
    table = exchange(total, SECOND)
    picked = call(
        pick_kernel, [VMEM, VMEM], VMEM, f32(MEMBERS, SENT, chunk), flops=10**8
    )(table, got)
    final = exchange(picked, FIRST)

    other_out = call(
        other_back_kernel, [SMEM, VMEM, VMEM, VMEM], VMEM, f32(ROWS, half), flops=10**9
    )(first_level, meta, back, final)
    swapped = lax.ppermute(other_out, "grp", swap)
    out = call(
        own_back_kernel, [SMEM, SMEM, VMEM, VMEM, VMEM], HBM, f32(ROWS, width),
        (pltpu.VMEM((MEMBERS, ROWS, chunk), jnp.float32), DMA((MEMBERS,))), flops=10**9,
    )(core, first_level, meta, back, final)
    out = call(
        place_kernel, [SMEM, VMEM, HBM], HBM, f32(ROWS, width), (DMA,), alias={2: 0}
    )(core, swapped, out)
    return out[None]


def solution(mesh):
    in_specs = (P("grp", "slab", None), P("grp"), P("grp"), P("grp", "slab"))
    out_specs = P("grp", "slab", None)
    return jax.shard_map(shards, mesh=mesh, in_specs=in_specs, out_specs=out_specs, check_vma=False)
```

```python
import functools

import jax
import jax.numpy as jnp
import numpy as np
from jax import lax
from jax.experimental import pallas as pl
from jax.experimental.pallas import tpu as pltpu
from jax.sharding import PartitionSpec as P

LEVEL_SUM = 9
LOW_LEVEL = 6
NY = 8
NZ = 8
MEMBERS = 4
ROWS = 128
PLANE = 8
BLOCK = 32
SLOTS = 7
THERE = SLOTS * BLOCK
FLAGS = THERE + PLANE
SENT = FLAGS + 8
ENTRY = 2 * (ROWS + PLANE)
TABLE = 8 * BLOCK + PLANE
LANES = 128
BLOCKS_OF = {6: (0, 1, 3, 4), 7: (0, 1, 2, 5), 8: (0, 2, 6, 7)}


def slots_of(levels):
    six, seven, eight = (level in levels for level in (6, 7, 8))
    third = 3 if six else (5 if seven else None)
    fifth = 6 if eight else (5 if six and seven else None)
    return (0, 1, 2, third, 4, fifth, 7)


def place_of(x, y):
    if x % 4 == 0 and y % 4 == 0:
        return (x // 4) * 2 + y // 4
    if x % 4 == 0 and y % 2 == 0:
        return 32 + (x // 4) * 2 + y // 4
    if x % 4 == 2 and y % 4 == 0:
        return 64 + (x // 4) * 2 + y // 4
    if x % 4 == 0:
        return 96 + (x // 4) * 4 + y // 2
    if x % 4 == 2:
        return 160 + (x // 4) * 2 + y // 4
    return 192 + (x // 2) * 2 + y // 4


def hier_line(n):
    h = np.zeros((n, n), np.float32)
    for j in range(n):
        h[j, j] += 1.0
        if j:
            s = j & -j
            h[j, j - s] -= 0.5
            h[j, (j + s) % n] -= 0.5
    return h


def dehier_line(n):
    e = np.zeros((n, n), np.float32)
    e[:, 0] = 1.0
    for k in range(1, n):
        for j in range(n):
            d = min(abs(j - k), n - abs(j - k))
            e[j, k] = max(0.0, 1.0 - d / (k & -k))
    return e


def one_grid(level, slots):
    n = 1 << (LEVEL_SUM - level)
    span = ROWS // n
    hy, ey = hier_line(n), dehier_line(n)
    forth = np.zeros((SENT, ROWS + PLANE), np.float32)
    back = np.zeros((ROWS, FLAGS), np.float32)
    for i in range(span):
        for y in range(n):
            t = place_of(i * 64 // span, y * 8 // n)
            m = BLOCK * slots.index(t // BLOCK) + t % BLOCK
            s = i & -i
            steps = [(i, 1.0)] + ([(i - s, -0.5), (i + s, -0.5)] if i else [])
            for j, w in steps:
                forth[m, j * n : j * n + n] += w * hy[y]
            for j in range(span):
                w = max(0.0, 1.0 - abs(j - i) / s) if i else 1.0 - j / span
                back[j * n : j * n + n, m] += w * ey[:, y]
    for y in range(n):
        t = THERE + y * 8 // n
        forth[t, ROWS : ROWS + n] += hy[y]
        for j in range(span):
            back[j * n : j * n + n, t] += j / span * ey[:, y]
    return forth, back


@functools.cache
def row_tables():
    forth, back = [], []
    for own in (6, 7, 8):
        for other in (6, 7, 8):
            slots = slots_of((own, other))
            mine, theirs = one_grid(own, slots), one_grid(other, slots)
            forth.append(np.concatenate([mine[0], theirs[0]], axis=1))
            back.append(mine[1])
    return np.stack(forth), np.stack(back)


def two_part_dot(table, values):
    high = values.astype(jnp.bfloat16)
    low = (values - high.astype(jnp.float32)).astype(jnp.bfloat16)
    dot = functools.partial(jnp.dot, preferred_element_type=jnp.float32)
    return dot(table, high) + dot(table, low)


def number_in(ref, row):
    return jnp.max(ref[row : row + 1, :LANES])


def core_here():
    return lax.axis_index("grp") % 2


def half_of(ref, core, rows=slice(None)):
    width = ref.shape[1] // 2
    return ref.at[rows, pl.ds(pl.multiple_of(core * width, LANES), width)]


def entry_kernel(level_ref, coeff_ref, rows_ref, out_ref, own_ref, other_ref):
    core = core_here()
    half = out_ref.shape[1]
    mine = pl.ds(pl.multiple_of(core * half, LANES), half)
    theirs = pl.ds(pl.multiple_of((1 - core) * half, LANES), half)
    own_ref[...] = rows_ref[:PLANE, mine]
    other_ref[...] = rows_ref[:PLANE, theirs]
    out_ref[:ROWS, :] = rows_ref[:, theirs]
    line = lax.broadcasted_iota(jnp.int32, (8, half), 0)
    out_ref[ROWS:, :] = jnp.where(line == 0, level_ref[0], coeff_ref[0]).astype(jnp.float32)


def forth_kernel(level_ref, coeff_ref, table_ref, rows_ref, own_next_ref, other_ref, other_next_ref, out_ref, meta_ref):
    own_level = level_ref[0]
    other_level = number_in(other_ref, ROWS).astype(jnp.int32)
    which = (own_level - LOW_LEVEL) * 3 + other_level - LOW_LEVEL
    chunk = out_ref.shape[2]
    lane = lax.broadcasted_iota(jnp.int32, (1, ENTRY), 1)
    scale = jnp.where(lane < ENTRY // 2, coeff_ref[0].astype(jnp.float32), number_in(other_ref, ROWS + 1))
    table = (table_ref[which].astype(jnp.float32) * scale).astype(jnp.bfloat16)
    six = jnp.logical_or(own_level == 6, other_level == 6).astype(jnp.float32)
    eight = jnp.logical_or(own_level == 8, other_level == 8).astype(jnp.float32)
    width = chunk // 2
    line = lax.broadcasted_iota(jnp.int32, (SENT - FLAGS, width), 0)
    flags = jnp.where(line == 0, six, eight)
    first = core_here() * MEMBERS * chunk
    for k in range(MEMBERS):
        for h in range(2):
            here = slice(h * width, (h + 1) * width)
            low = k * chunk + h * width
            span = slice(low, low + width)
            own = rows_ref[:, pl.ds(pl.multiple_of(first + low, LANES), width)]
            values = jnp.concatenate(
                [own, own_next_ref[:, span], other_ref[:ROWS, span], other_next_ref[:, span]], axis=0
            )
            out_ref[k, :, here] = two_part_dot(table, values)
            out_ref[k, FLAGS:SENT, here] = flags
    meta_ref[...] = other_ref[ROWS:, :LANES]


def add_kernel(got_ref, out_ref):
    for j in range(MEMBERS):
        lanes = slice(j * LANES, (j + 1) * LANES)
        six = [got_ref[k, FLAGS : FLAGS + 1, lanes] == 1.0 for k in range(MEMBERS)]
        eight = [got_ref[k, FLAGS + 1 : FLAGS + 2, lanes] == 1.0 for k in range(MEMBERS)]
        slot = lambda k, i: got_ref[k, BLOCK * i : BLOCK * (i + 1), lanes]
        terms = (
            lambda k: slot(k, 0),
            lambda k: slot(k, 1),
            lambda k: slot(k, 2),
            lambda k: jnp.where(six[k], slot(k, 3), 0.0),
            lambda k: slot(k, 4),
            lambda k: jnp.where(six[k], jnp.where(eight[k], 0.0, slot(k, 5)), slot(k, 3)),
            lambda k: jnp.where(eight[k], slot(k, 5), 0.0),
            lambda k: slot(k, 6),
            lambda k: got_ref[k, THERE:FLAGS, lanes],
        )
        for block, term in enumerate(terms):
            total = term(0)
            for k in range(1, MEMBERS):
                total = total + term(k)
            out_ref[j, BLOCK * block : BLOCK * block + total.shape[0], :] = total


def total_kernel(got_ref, out_ref):
    total = got_ref[0]
    for k in range(1, MEMBERS):
        total = total + got_ref[k]
    for k in range(MEMBERS):
        out_ref[k] = total


def pick_kernel(table_ref, got_ref, out_ref):
    for j in range(MEMBERS):
        lanes = slice(j * LANES, (j + 1) * LANES)
        block = lambda i: table_ref[j, BLOCK * i : BLOCK * (i + 1), :]
        for k in range(MEMBERS):
            six = got_ref[k, FLAGS : FLAGS + 1, lanes] == 1.0
            eight = got_ref[k, FLAGS + 1 : FLAGS + 2, lanes] == 1.0
            out_ref[k, 0:32, lanes] = block(0)
            out_ref[k, 32:64, lanes] = block(1)
            out_ref[k, 64:96, lanes] = block(2)
            out_ref[k, 96:128, lanes] = jnp.where(six, block(3), block(5))
            out_ref[k, 128:160, lanes] = block(4)
            out_ref[k, 160:192, lanes] = jnp.where(eight, block(6), block(5))
            out_ref[k, 192:224, lanes] = block(7)
            out_ref[k, THERE:FLAGS, lanes] = table_ref[j, 8 * BLOCK : TABLE, :]


def levels_in(level_ref, meta_ref):
    return level_ref[0] - LOW_LEVEL, number_in(meta_ref, 0).astype(jnp.int32) - LOW_LEVEL


def pieces(ref):
    width = ref.shape[2] // 2
    for k in range(MEMBERS):
        for h in range(2):
            yield ref[k, :, h * width : (h + 1) * width]


def other_back_kernel(level_ref, meta_ref, table_ref, got_ref, out_ref):
    own, other = levels_in(level_ref, meta_ref)
    table = table_ref[other * 3 + own]
    for i, values in enumerate(pieces(got_ref)):
        width = values.shape[1]
        out_ref[:, i * width : (i + 1) * width] = two_part_dot(table, values)


def own_back_kernel(level_ref, meta_ref, table_ref, got_ref, out_ref, done_ref, sems):
    own, other = levels_in(level_ref, meta_ref)
    table = table_ref[own * 3 + other]
    first = core_here() * 2 * MEMBERS
    copies = []
    for i, values in enumerate(pieces(got_ref)):
        width = values.shape[1]
        done_ref[i] = two_part_dot(table, values)
        start = pl.multiple_of((first + i) * width, LANES)
        copy = pltpu.make_async_copy(done_ref.at[i], out_ref.at[:, pl.ds(start, width)], sems.at[i])
        copy.start()
        copies.append(copy)
    for copy in copies:
        copy.wait()


def place_kernel(values_ref, filled_ref, out_ref, sem):
    copy = pltpu.make_async_copy(values_ref, half_of(out_ref, 1 - core_here()), sem)
    copy.start()
    copy.wait()


def member(y, z, core):
    return (y % NY * NZ + z % NZ) * 2 + core


TILES = [
    [member(2 * a + i + core, 2 * b + j + core, core) for i in (0, 1) for j in (0, 1)]
    for core in (0, 1)
    for a in range(NY // 2)
    for b in range(NZ // 2)
]
ALONG_Y = [[[member(2 * a + i, z, core) for a in range(NY // 2)] for i in (0, 1) for z in range(NZ)] for core in (0, 1)]
ALONG_Z = [[[member(y, 2 * b + j, core) for b in range(NZ // 2)] for j in (0, 1) for y in range(NY)] for core in (0, 1)]
LINES = ALONG_Y[0] + ALONG_Z[1]
OTHER_LINES = ALONG_Z[0] + ALONG_Y[1]
VMEM = pl.BlockSpec(memory_space=pltpu.VMEM)
SMEM = pl.BlockSpec(memory_space=pltpu.SMEM)
HBM = pl.BlockSpec(memory_space=pltpu.HBM)
DMA = pltpu.SemaphoreType.DMA


def exchange(values, groups):
    return lax.all_to_all(values, "grp", 0, 0, axis_index_groups=groups, tiled=True)


def f32(*shape):
    return jax.ShapeDtypeStruct(shape, jnp.float32)


def call(kernel, name, ins, outs, shapes, scratch=(), limit=16, flops=0, moved=0, alias=None):
    return pl.pallas_call(
        kernel,
        in_specs=ins,
        out_specs=outs,
        out_shape=shapes,
        scratch_shapes=scratch,
        compiler_params=pltpu.CompilerParams(vmem_limit_bytes=limit << 20),
        cost_estimate=pl.CostEstimate(flops=flops, bytes_accessed=moved, transcendentals=0),
        input_output_aliases=alias or {},
        name=name,
    )


def shards(grids, first_level, coeffs, slot_map):
    rows = grids[0]
    width = rows.shape[1]
    half = width // 2
    chunk = half // MEMBERS
    slabs = lax.axis_size("slab")
    members = lax.axis_size("grp")
    swap = [(i, i ^ 1) for i in range(members)]
    forth, back = (jnp.asarray(table, jnp.bfloat16) for table in row_tables())

    def to_previous(values, turn):
        pairs = [
            (g * slabs + s, (g ^ turn) * slabs + (s - 1) % slabs)
            for g in range(members)
            for s in range(slabs)
        ]
        return lax.ppermute(values, ("grp", "slab"), pairs)

    entry, own_plane, other_plane = call(
        entry_kernel, "entry", [SMEM, SMEM, VMEM], [VMEM] * 3,
        [f32(ROWS + 8, half), f32(PLANE, half), f32(PLANE, half)],
    )(first_level, coeffs, rows)
    other_next = to_previous(other_plane, 1)
    own_next = to_previous(own_plane, 0)
    other = lax.ppermute(entry, "grp", swap)
    sent, meta = call(
        forth_kernel, "forth", [SMEM, SMEM] + [VMEM] * 5, [VMEM, VMEM],
        [f32(MEMBERS, SENT, chunk), f32(8, LANES)], flops=10**9,
    )(first_level, coeffs, forth, rows, own_next, other, other_next)
    got = exchange(sent, TILES)

    parts = call(add_kernel, "add", [VMEM], VMEM, f32(MEMBERS, TABLE, LANES), flops=10**8)(got)
    for groups in (LINES, OTHER_LINES):
        parts = exchange(parts, groups)
        parts = call(total_kernel, "total", [VMEM], VMEM, f32(MEMBERS, TABLE, LANES), flops=10**8)(parts)
    table = exchange(parts, LINES)
    picked = call(
        pick_kernel, "pick", [VMEM, VMEM], VMEM, f32(MEMBERS, FLAGS, chunk), flops=10**8
    )(table, got)
    final = exchange(picked, TILES)

    other_out = call(
        other_back_kernel, "other_back", [SMEM, VMEM, VMEM, VMEM], VMEM, f32(ROWS, half), flops=10**9
    )(first_level, meta, back, final)
    swapped = lax.ppermute(other_out, "grp", swap)
    out = call(
        own_back_kernel, "own_back", [SMEM, VMEM, VMEM, VMEM], HBM, f32(ROWS, width),
        (pltpu.VMEM((2 * MEMBERS, ROWS, chunk // 2), jnp.float32), DMA((2 * MEMBERS,))), flops=10**9,
    )(first_level, meta, back, final)
    out = call(
        place_kernel, "place", [VMEM, HBM], HBM, f32(ROWS, width), (DMA,), alias={1: 0}
    )(swapped, out)
    return out[None]


def solution(mesh):
    in_specs = (P("grp", "slab", None), P("grp"), P("grp"), P("grp", "slab"))
    out_specs = P("grp", "slab", None)
    return jax.shard_map(shards, mesh=mesh, in_specs=in_specs, out_specs=out_specs, check_vma=False)
```

```python
import functools

import jax
import jax.numpy as jnp
import numpy as np
from jax import lax
from jax.experimental import pallas as pl
from jax.experimental.pallas import tpu as pltpu
from jax.sharding import PartitionSpec as P

LEVEL_SUM = 9
LOW_LEVEL = 6
NY = 8
NZ = 8
MEMBERS = 4
ROWS = 128
PLANE = 8
BLOCK = 32
SLOTS = 7
THERE = SLOTS * BLOCK
FLAGS = THERE + PLANE
SENT = FLAGS + 8
ENTRY = 2 * (ROWS + PLANE)
TABLE = 8 * BLOCK + PLANE
LANES = 128


def slots_of(levels):
    six, seven, eight = (level in levels for level in (6, 7, 8))
    third = 3 if six else (5 if seven else None)
    fifth = 6 if eight else (5 if six and seven else None)
    return (0, 1, 2, third, 4, fifth, 7)


def place_of(x, y):
    if x % 4 == 0 and y % 4 == 0:
        return (x // 4) * 2 + y // 4
    if x % 4 == 0 and y % 2 == 0:
        return 32 + (x // 4) * 2 + y // 4
    if x % 4 == 2 and y % 4 == 0:
        return 64 + (x // 4) * 2 + y // 4
    if x % 4 == 0:
        return 96 + (x // 4) * 4 + y // 2
    if x % 4 == 2:
        return 160 + (x // 4) * 2 + y // 4
    return 192 + (x // 2) * 2 + y // 4


def hier_line(n):
    h = np.zeros((n, n), np.float32)
    for j in range(n):
        h[j, j] += 1.0
        if j:
            s = j & -j
            h[j, j - s] -= 0.5
            h[j, (j + s) % n] -= 0.5
    return h


def dehier_line(n):
    e = np.zeros((n, n), np.float32)
    e[:, 0] = 1.0
    for k in range(1, n):
        for j in range(n):
            d = min(abs(j - k), n - abs(j - k))
            e[j, k] = max(0.0, 1.0 - d / (k & -k))
    return e


def one_grid(level, slots):
    n = 1 << (LEVEL_SUM - level)
    span = ROWS // n
    hy, ey = hier_line(n), dehier_line(n)
    forth = np.zeros((SENT, ROWS + PLANE), np.float32)
    back = np.zeros((ROWS, FLAGS), np.float32)
    for i in range(span):
        for y in range(n):
            t = place_of(i * 64 // span, y * 8 // n)
            m = BLOCK * slots.index(t // BLOCK) + t % BLOCK
            s = i & -i
            steps = [(i, 1.0)] + ([(i - s, -0.5), (i + s, -0.5)] if i else [])
            for j, w in steps:
                forth[m, j * n : j * n + n] += w * hy[y]
            for j in range(span):
                w = max(0.0, 1.0 - abs(j - i) / s) if i else 1.0 - j / span
                back[j * n : j * n + n, m] += w * ey[:, y]
    for y in range(n):
        t = THERE + y * 8 // n
        forth[t, ROWS : ROWS + n] += hy[y]
        for j in range(span):
            back[j * n : j * n + n, t] += j / span * ey[:, y]
    return forth, back


@functools.cache
def row_tables():
    forth, back = [], []
    for own in (6, 7, 8):
        for other in (6, 7, 8):
            slots = slots_of((own, other))
            mine, theirs = one_grid(own, slots), one_grid(other, slots)
            forth.append(np.concatenate([mine[0], theirs[0]], axis=1))
            back.append(mine[1])
    return np.stack(forth), np.stack(back)


def two_part_dot(table, values):
    high = values.astype(jnp.bfloat16)
    low = (values - high.astype(jnp.float32)).astype(jnp.bfloat16)
    dot = functools.partial(jnp.dot, preferred_element_type=jnp.float32)
    return dot(table, high) + dot(table, low)


def number_in(ref, row):
    return jnp.max(ref[row : row + 1, :LANES])


def core_here():
    return lax.axis_index("grp") % 2


def piece_here(turn):
    me = lax.axis_index("grp")
    core, z, y = me % 2, me // 2 % NZ, me // (2 * NZ)
    return ((y + core) % 2 * 2 + (z + core) % 2) ^ turn


def half_of(ref, core, rows=slice(None)):
    width = ref.shape[1] // 2
    return ref.at[rows, pl.ds(pl.multiple_of(core * width, LANES), width)]


def entry_kernel(level_ref, coeff_ref, rows_ref, out_ref, own_ref, other_ref):
    core = core_here()
    half = out_ref.shape[1]
    mine = pl.ds(pl.multiple_of(core * half, LANES), half)
    theirs = pl.ds(pl.multiple_of((1 - core) * half, LANES), half)
    own_ref[...] = rows_ref[:PLANE, mine]
    other_ref[...] = rows_ref[:PLANE, theirs]
    out_ref[:ROWS, :] = rows_ref[:, theirs]
    line = lax.broadcasted_iota(jnp.int32, (8, half), 0)
    out_ref[ROWS:, :] = jnp.where(line == 0, level_ref[...], coeff_ref[...]).astype(jnp.float32)


def forth_kernel(level_ref, coeff_ref, table_ref, rows_ref, own_next_ref, other_ref, other_next_ref, *outs):
    *out_refs, meta_ref = outs
    own_level = level_ref[0]
    other_level = number_in(other_ref, ROWS).astype(jnp.int32)
    which = (own_level - LOW_LEVEL) * 3 + other_level - LOW_LEVEL
    chunk = out_refs[0].shape[1]
    lane = lax.broadcasted_iota(jnp.int32, (1, ENTRY), 1)
    scale = jnp.where(lane < ENTRY // 2, coeff_ref[0].astype(jnp.float32), number_in(other_ref, ROWS + 1))
    table = (table_ref[which].astype(jnp.float32) * scale).astype(jnp.bfloat16)
    six = jnp.logical_or(own_level == 6, other_level == 6).astype(jnp.float32)
    eight = jnp.logical_or(own_level == 8, other_level == 8).astype(jnp.float32)
    width = chunk // 2
    line = lax.broadcasted_iota(jnp.int32, (SENT - FLAGS, width), 0)
    flags = jnp.where(line == 0, six, eight)
    first = core_here() * MEMBERS * chunk
    for turn, out_ref in enumerate(out_refs):
        for h in range(2):
            here = slice(h * width, (h + 1) * width)
            low = piece_here(turn) * chunk + h * width
            span = pl.ds(pl.multiple_of(low, LANES), width)
            own = rows_ref[:, pl.ds(pl.multiple_of(first + low, LANES), width)]
            values = jnp.concatenate(
                [own, own_next_ref[:, span], other_ref[:ROWS, span], other_next_ref[:, span]], axis=0
            )
            out_ref[:, here] = two_part_dot(table, values)
            out_ref[FLAGS:SENT, here] = flags
    meta_ref[...] = other_ref[ROWS:, :LANES]


def add_kernel(*refs):
    *got_refs, out_ref = refs
    for j in range(MEMBERS):
        lanes = slice(j * LANES, (j + 1) * LANES)
        six = [ref[FLAGS : FLAGS + 1, lanes] == 1.0 for ref in got_refs]
        eight = [ref[FLAGS + 1 : FLAGS + 2, lanes] == 1.0 for ref in got_refs]
        slot = lambda k, i: got_refs[k][BLOCK * i : BLOCK * (i + 1), lanes]
        terms = (
            lambda k: slot(k, 0),
            lambda k: slot(k, 1),
            lambda k: slot(k, 2),
            lambda k: jnp.where(six[k], slot(k, 3), 0.0),
            lambda k: slot(k, 4),
            lambda k: jnp.where(six[k], jnp.where(eight[k], 0.0, slot(k, 5)), slot(k, 3)),
            lambda k: jnp.where(eight[k], slot(k, 5), 0.0),
            lambda k: slot(k, 6),
            lambda k: got_refs[k][THERE:FLAGS, lanes],
        )
        for block, term in enumerate(terms):
            total = term(0)
            for k in range(1, MEMBERS):
                total = total + term(k)
            out_ref[j, BLOCK * block : BLOCK * block + total.shape[0], :] = total


def total_kernel(got_ref, out_ref):
    total = got_ref[0]
    for k in range(1, MEMBERS):
        total = total + got_ref[k]
    for k in range(MEMBERS):
        out_ref[k] = total


def pick_kernel(table_ref, *refs):
    for got_ref, out_ref in zip(refs[:MEMBERS], refs[MEMBERS:]):
        for j in range(MEMBERS):
            lanes = slice(j * LANES, (j + 1) * LANES)
            block = lambda i: table_ref[j, BLOCK * i : BLOCK * (i + 1), :]
            six = got_ref[FLAGS : FLAGS + 1, lanes] == 1.0
            eight = got_ref[FLAGS + 1 : FLAGS + 2, lanes] == 1.0
            out_ref[0:32, lanes] = block(0)
            out_ref[32:64, lanes] = block(1)
            out_ref[64:96, lanes] = block(2)
            out_ref[96:128, lanes] = jnp.where(six, block(3), block(5))
            out_ref[128:160, lanes] = block(4)
            out_ref[160:192, lanes] = jnp.where(eight, block(6), block(5))
            out_ref[192:224, lanes] = block(7)
            out_ref[THERE:FLAGS, lanes] = table_ref[j, 8 * BLOCK : TABLE, :]


def levels_in(level_ref, meta_ref):
    return level_ref[0] - LOW_LEVEL, number_in(meta_ref, 0).astype(jnp.int32) - LOW_LEVEL


def pieces(refs):
    for turn, ref in enumerate(refs):
        chunk = ref.shape[1]
        for h in range(2):
            width = chunk // 2
            yield piece_here(turn) * chunk + h * width, ref[:, h * width : (h + 1) * width]


def other_back_kernel(level_ref, meta_ref, table_ref, *refs):
    *got_refs, out_ref = refs
    own, other = levels_in(level_ref, meta_ref)
    table = table_ref[other * 3 + own]
    for low, values in pieces(got_refs):
        out_ref[:, pl.ds(pl.multiple_of(low, LANES), values.shape[1])] = two_part_dot(table, values)


def own_back_kernel(level_ref, meta_ref, table_ref, *refs):
    *got_refs, out_ref, done_ref, sems = refs
    own, other = levels_in(level_ref, meta_ref)
    table = table_ref[own * 3 + other]
    first = core_here() * (out_ref.shape[1] // 2)
    copies = []
    for i, (low, values) in enumerate(pieces(got_refs)):
        width = values.shape[1]
        done_ref[i] = two_part_dot(table, values)
        start = pl.multiple_of(first + low, LANES)
        copy = pltpu.make_async_copy(done_ref.at[i], out_ref.at[:, pl.ds(start, width)], sems.at[i])
        copy.start()
        copies.append(copy)
    for copy in copies:
        copy.wait()


def place_kernel(values_ref, filled_ref, out_ref, sem):
    copy = pltpu.make_async_copy(values_ref, half_of(out_ref, 1 - core_here()), sem)
    copy.start()
    copy.wait()


def member(y, z, core):
    return (y % NY * NZ + z % NZ) * 2 + core


TILES = [
    [member(2 * a + i + core, 2 * b + j + core, core) for i in (0, 1) for j in (0, 1)]
    for core in (0, 1)
    for a in range(NY // 2)
    for b in range(NZ // 2)
]
ALONG_Y = [[[member(2 * a + i, z, core) for a in range(NY // 2)] for i in (0, 1) for z in range(NZ)] for core in (0, 1)]
ALONG_Z = [[[member(y, 2 * b + j, core) for b in range(NZ // 2)] for j in (0, 1) for y in range(NY)] for core in (0, 1)]
LINES = ALONG_Y[0] + ALONG_Z[1]
OTHER_LINES = ALONG_Z[0] + ALONG_Y[1]
VMEM = pl.BlockSpec(memory_space=pltpu.VMEM)
SMEM = pl.BlockSpec(memory_space=pltpu.SMEM)
HBM = pl.BlockSpec(memory_space=pltpu.HBM)
DMA = pltpu.SemaphoreType.DMA


def exchange(values, groups):
    return lax.all_to_all(values, "grp", 0, 0, axis_index_groups=groups, tiled=True)


def f32(*shape):
    return jax.ShapeDtypeStruct(shape, jnp.float32)


def call(kernel, ins, outs, shapes, scratch=(), limit=16, flops=0, moved=0, alias=None):
    return pl.pallas_call(
        kernel,
        in_specs=ins,
        out_specs=outs,
        out_shape=shapes,
        scratch_shapes=scratch,
        compiler_params=pltpu.CompilerParams(vmem_limit_bytes=limit << 20),
        cost_estimate=pl.CostEstimate(flops=flops, bytes_accessed=moved, transcendentals=0),
        input_output_aliases=alias or {},
    )


def shards(grids, first_level, coeffs, slot_map):
    rows = grids[0]
    width = rows.shape[1]
    half = width // 2
    chunk = half // MEMBERS
    slabs = lax.axis_size("slab")
    members = lax.axis_size("grp")
    swap = [(i, i ^ 1) for i in range(members)]
    forth, back = (jnp.asarray(table, jnp.bfloat16) for table in row_tables())

    def to_previous(values, turn):
        pairs = [
            (g * slabs + s, (g ^ turn) * slabs + (s - 1) % slabs)
            for g in range(members)
            for s in range(slabs)
        ]
        return lax.ppermute(values, ("grp", "slab"), pairs)

    def through_tile(pieces):
        turned = lambda turn: [(tile[i], tile[i ^ turn]) for tile in TILES for i in range(MEMBERS)]
        far = {}
        for turn in (3, 2, 1):
            far[turn] = lax.ppermute(pieces[turn], "grp", turned(turn))
        return [pieces[0], far[1], far[2], far[3]]

    entry, own_plane, other_plane = call(
        entry_kernel, [VMEM] * 3, [VMEM] * 3,
        [f32(ROWS + 8, half), f32(PLANE, half), f32(PLANE, half)],
    )(first_level[None], coeffs[None], rows)
    other_next = to_previous(other_plane, 1)
    own_next = to_previous(own_plane, 0)
    other = lax.ppermute(entry, "grp", swap)
    *sent, meta = call(
        forth_kernel, [SMEM, SMEM] + [VMEM] * 5, [VMEM] * (MEMBERS + 1),
        [f32(SENT, chunk)] * MEMBERS + [f32(8, LANES)], flops=10**9,
    )(first_level, coeffs, forth, rows, own_next, other, other_next)
    got = through_tile(sent)

    parts = call(add_kernel, [VMEM] * MEMBERS, VMEM, f32(MEMBERS, TABLE, LANES), flops=10**8)(*got)
    for groups in (LINES, OTHER_LINES):
        parts = exchange(parts, groups)
        parts = call(total_kernel, [VMEM], VMEM, f32(MEMBERS, TABLE, LANES), flops=10**8)(parts)
    table = exchange(parts, LINES)
    picked = call(
        pick_kernel, [VMEM] * (MEMBERS + 1), [VMEM] * MEMBERS, [f32(FLAGS, chunk)] * MEMBERS, flops=10**8
    )(table, *got)
    final = through_tile(picked)

    other_out = call(
        other_back_kernel, [SMEM] + [VMEM] * (MEMBERS + 2), VMEM, f32(ROWS, half), flops=10**9
    )(first_level, meta, back, *final)
    swapped = lax.ppermute(other_out, "grp", swap)
    out = call(
        own_back_kernel, [SMEM] + [VMEM] * (MEMBERS + 2), HBM, f32(ROWS, width),
        (pltpu.VMEM((2 * MEMBERS, ROWS, chunk // 2), jnp.float32), DMA((2 * MEMBERS,))), flops=10**9,
    )(first_level, meta, back, *final)
    out = call(place_kernel, [VMEM, HBM], HBM, f32(ROWS, width), (DMA,), alias={1: 0})(swapped, out)
    return out[None]


def solution(mesh):
    in_specs = (P("grp", "slab", None), P("grp"), P("grp"), P("grp", "slab"))
    out_specs = P("grp", "slab", None)
    return jax.shard_map(shards, mesh=mesh, in_specs=in_specs, out_specs=out_specs, check_vma=False)
```

```python
import functools

import jax
import jax.numpy as jnp
import numpy as np
from jax import lax
from jax.experimental import pallas as pl
from jax.experimental.pallas import tpu as pltpu
from jax.sharding import PartitionSpec as P

LEVEL_SUM = 9
LOW_LEVEL = 6
NY = 8
NZ = 8
MEMBERS = 4
ROWS = 128
PLANE = 8
BLOCK = 32
SLOTS = 7
THERE = SLOTS * BLOCK
FLAGS = THERE + PLANE
SENT = FLAGS + 8
ENTRY = 2 * (ROWS + PLANE)
TABLE = 8 * BLOCK + PLANE
LANES = 128
SHARE = 16


def slots_of(levels):
    six, seven, eight = (level in levels for level in (6, 7, 8))
    third = 3 if six else (5 if seven else None)
    fifth = 6 if eight else (5 if six and seven else None)
    return (0, 1, 2, third, 4, fifth, 7)


def place_of(x, y):
    if x % 4 == 0 and y % 4 == 0:
        return (x // 4) * 2 + y // 4
    if x % 4 == 0 and y % 2 == 0:
        return 32 + (x // 4) * 2 + y // 4
    if x % 4 == 2 and y % 4 == 0:
        return 64 + (x // 4) * 2 + y // 4
    if x % 4 == 0:
        return 96 + (x // 4) * 4 + y // 2
    if x % 4 == 2:
        return 160 + (x // 4) * 2 + y // 4
    return 192 + (x // 2) * 2 + y // 4


def hier_line(n):
    h = np.zeros((n, n), np.float32)
    for j in range(n):
        h[j, j] += 1.0
        if j:
            s = j & -j
            h[j, j - s] -= 0.5
            h[j, (j + s) % n] -= 0.5
    return h


def dehier_line(n):
    e = np.zeros((n, n), np.float32)
    e[:, 0] = 1.0
    for k in range(1, n):
        for j in range(n):
            d = min(abs(j - k), n - abs(j - k))
            e[j, k] = max(0.0, 1.0 - d / (k & -k))
    return e


def one_grid(level, slots):
    n = 1 << (LEVEL_SUM - level)
    span = ROWS // n
    hy, ey = hier_line(n), dehier_line(n)
    forth = np.zeros((SENT, ROWS + PLANE), np.float32)
    back = np.zeros((ROWS, FLAGS), np.float32)
    for i in range(span):
        for y in range(n):
            t = place_of(i * 64 // span, y * 8 // n)
            m = BLOCK * slots.index(t // BLOCK) + t % BLOCK
            s = i & -i
            steps = [(i, 1.0)] + ([(i - s, -0.5), (i + s, -0.5)] if i else [])
            for j, w in steps:
                forth[m, j * n : j * n + n] += w * hy[y]
            for j in range(span):
                w = max(0.0, 1.0 - abs(j - i) / s) if i else 1.0 - j / span
                back[j * n : j * n + n, m] += w * ey[:, y]
    for y in range(n):
        t = THERE + y * 8 // n
        forth[t, ROWS : ROWS + n] += hy[y]
        for j in range(span):
            back[j * n : j * n + n, t] += j / span * ey[:, y]
    return forth, back


@functools.cache
def row_tables():
    forth, back = [], []
    for own in (6, 7, 8):
        for other in (6, 7, 8):
            slots = slots_of((own, other))
            mine, theirs = one_grid(own, slots), one_grid(other, slots)
            forth.append(np.concatenate([mine[0], theirs[0]], axis=1))
            back.append(mine[1])
    return np.stack(forth), np.stack(back)


def two_part_dot(table, values):
    high = values.astype(jnp.bfloat16)
    low = (values - high.astype(jnp.float32)).astype(jnp.bfloat16)
    dot = functools.partial(jnp.dot, preferred_element_type=jnp.float32)
    return dot(table, high) + dot(table, low)


def number_in(ref, row):
    return jnp.max(ref[row : row + 1, :LANES])


def core_here():
    return lax.axis_index("grp") % 2


def piece_here(turn):
    me = lax.axis_index("grp")
    core, z, y = me % 2, me // 2 % NZ, me // (2 * NZ)
    return ((y + core) % 2 * 2 + (z + core) % 2) ^ turn


def half_of(ref, core, rows=slice(None)):
    width = ref.shape[1] // 2
    return ref.at[rows, pl.ds(pl.multiple_of(core * width, LANES), width)]


def entry_kernel(rows_ref, out_ref, own_plane_ref, other_plane_ref):
    core = core_here()
    half = out_ref.shape[1]
    mine = pl.ds(pl.multiple_of(core * half, LANES), half)
    theirs = pl.ds(pl.multiple_of((1 - core) * half, LANES), half)
    own_plane_ref[...] = rows_ref[:PLANE, mine]
    other_plane_ref[...] = rows_ref[:PLANE, theirs]
    out_ref[:ROWS, :] = rows_ref[:, theirs]


def stamp_kernel(level_ref, coeff_ref, rows_ref, out_ref):
    line = lax.broadcasted_iota(jnp.int32, (8, out_ref.shape[1]), 0)
    out_ref[ROWS:, :] = jnp.where(line == 0, level_ref[0], coeff_ref[0]).astype(jnp.float32)


def forth_kernel(turns, level_ref, coeff_ref, table_ref, rows_ref, own_next_ref, other_ref, other_next_ref, *out_refs):
    own_level = level_ref[0]
    other_level = number_in(other_ref, ROWS).astype(jnp.int32)
    which = (own_level - LOW_LEVEL) * 3 + other_level - LOW_LEVEL
    chunk = out_refs[0].shape[1]
    lane = lax.broadcasted_iota(jnp.int32, (1, ENTRY), 1)
    scale = jnp.where(lane < ENTRY // 2, coeff_ref[0].astype(jnp.float32), number_in(other_ref, ROWS + 1))
    table = (table_ref[which].astype(jnp.float32) * scale).astype(jnp.bfloat16)
    six = jnp.logical_or(own_level == 6, other_level == 6).astype(jnp.float32)
    eight = jnp.logical_or(own_level == 8, other_level == 8).astype(jnp.float32)
    width = chunk // 2
    line = lax.broadcasted_iota(jnp.int32, (SENT - FLAGS, width), 0)
    flags = jnp.where(line == 0, six, eight)
    first = core_here() * MEMBERS * chunk
    for turn, out_ref in zip(turns, out_refs):
        for h in range(2):
            here = slice(h * width, (h + 1) * width)
            low = piece_here(turn) * chunk + h * width
            span = pl.ds(pl.multiple_of(low, LANES), width)
            own = rows_ref[:, pl.ds(pl.multiple_of(first + low, LANES), width)]
            values = jnp.concatenate(
                [own, own_next_ref[:, span], other_ref[:ROWS, span], other_next_ref[:, span]], axis=0
            )
            out_ref[:, here] = two_part_dot(table, values)
            out_ref[FLAGS:SENT, here] = flags


def meta_kernel(other_ref, meta_ref):
    meta_ref[...] = other_ref[ROWS:, :LANES]


def add_kernel(*refs):
    *got_refs, out_ref = refs
    for j in range(MEMBERS):
        lanes = slice(j * LANES, (j + 1) * LANES)
        six = [ref[FLAGS : FLAGS + 1, lanes] == 1.0 for ref in got_refs]
        eight = [ref[FLAGS + 1 : FLAGS + 2, lanes] == 1.0 for ref in got_refs]
        slot = lambda k, i: got_refs[k][BLOCK * i : BLOCK * (i + 1), lanes]
        terms = (
            lambda k: slot(k, 0),
            lambda k: slot(k, 1),
            lambda k: slot(k, 2),
            lambda k: jnp.where(six[k], slot(k, 3), 0.0),
            lambda k: slot(k, 4),
            lambda k: jnp.where(six[k], jnp.where(eight[k], 0.0, slot(k, 5)), slot(k, 3)),
            lambda k: jnp.where(eight[k], slot(k, 5), 0.0),
            lambda k: slot(k, 6),
            lambda k: got_refs[k][THERE:FLAGS, lanes],
        )
        for block, term in enumerate(terms):
            total = term(0)
            for k in range(1, MEMBERS):
                total = total + term(k)
            out_ref[j, BLOCK * block : BLOCK * block + total.shape[0], :] = total


def total_kernel(got_ref, out_ref):
    total = got_ref[0]
    for k in range(1, MEMBERS):
        total = total + got_ref[k]
    for k in range(MEMBERS):
        out_ref[k] = total


def pick_kernel(table_ref, *refs):
    for got_ref, out_ref in zip(refs[:MEMBERS], refs[MEMBERS:]):
        for j in range(MEMBERS):
            lanes = slice(j * LANES, (j + 1) * LANES)
            block = lambda i: table_ref[j, BLOCK * i : BLOCK * (i + 1), :]
            six = got_ref[FLAGS : FLAGS + 1, lanes] == 1.0
            eight = got_ref[FLAGS + 1 : FLAGS + 2, lanes] == 1.0
            out_ref[0:32, lanes] = block(0)
            out_ref[32:64, lanes] = block(1)
            out_ref[64:96, lanes] = block(2)
            out_ref[96:128, lanes] = jnp.where(six, block(3), block(5))
            out_ref[128:160, lanes] = block(4)
            out_ref[160:192, lanes] = jnp.where(eight, block(6), block(5))
            out_ref[192:224, lanes] = block(7)
            out_ref[THERE:FLAGS, lanes] = table_ref[j, 8 * BLOCK : TABLE, :]


def levels_in(level_ref, meta_ref):
    return level_ref[0] - LOW_LEVEL, number_in(meta_ref, 0).astype(jnp.int32) - LOW_LEVEL


def pieces(refs):
    for turn, ref in enumerate(refs):
        chunk = ref.shape[1]
        for h in range(2):
            width = chunk // 2
            yield piece_here(turn) * chunk + h * width, ref[:, h * width : (h + 1) * width]


def other_back_kernel(level_ref, meta_ref, table_ref, *refs):
    *got_refs, out_ref = refs
    own, other = levels_in(level_ref, meta_ref)
    table = table_ref[other * 3 + own]
    for low, values in pieces(got_refs):
        out_ref[:, pl.ds(pl.multiple_of(low, LANES), values.shape[1])] = two_part_dot(table, values)


def own_back_kernel(level_ref, meta_ref, table_ref, *refs):
    *got_refs, out_ref, done_ref, sems = refs
    own, other = levels_in(level_ref, meta_ref)
    table = table_ref[own * 3 + other]
    first = core_here() * (out_ref.shape[1] // 2)
    copies = []
    for i, (low, values) in enumerate(pieces(got_refs)):
        width = values.shape[1]
        done_ref[i] = two_part_dot(table, values)
        start = pl.multiple_of(first + low, LANES)
        copy = pltpu.make_async_copy(done_ref.at[i], out_ref.at[:, pl.ds(start, width)], sems.at[i])
        copy.start()
        copies.append(copy)
    for copy in copies:
        copy.wait()


def place_kernel(values_ref, filled_ref, out_ref, sems):
    copies = []
    for i in range(ROWS // SHARE):
        part = slice(i * SHARE, (i + 1) * SHARE)
        to = half_of(out_ref, 1 - core_here(), part)
        copies.append(pltpu.make_async_copy(values_ref.at[part], to, sems.at[i]))
    for copy in copies:
        copy.start()
    for copy in copies:
        copy.wait()


def member(y, z, core):
    return (y % NY * NZ + z % NZ) * 2 + core


TILES = [
    [member(2 * a + i + core, 2 * b + j + core, core) for i in (0, 1) for j in (0, 1)]
    for core in (0, 1)
    for a in range(NY // 2)
    for b in range(NZ // 2)
]
ALONG_Y = [[[member(2 * a + i, z, core) for a in range(NY // 2)] for i in (0, 1) for z in range(NZ)] for core in (0, 1)]
ALONG_Z = [[[member(y, 2 * b + j, core) for b in range(NZ // 2)] for j in (0, 1) for y in range(NY)] for core in (0, 1)]
LINES = ALONG_Y[0] + ALONG_Z[1]
OTHER_LINES = ALONG_Z[0] + ALONG_Y[1]
VMEM = pl.BlockSpec(memory_space=pltpu.VMEM)
SMEM = pl.BlockSpec(memory_space=pltpu.SMEM)
HBM = pl.BlockSpec(memory_space=pltpu.HBM)
DMA = pltpu.SemaphoreType.DMA


def exchange(values, groups):
    return lax.all_to_all(values, "grp", 0, 0, axis_index_groups=groups, tiled=True)


def f32(*shape):
    return jax.ShapeDtypeStruct(shape, jnp.float32)


def call(kernel, ins, outs, shapes, scratch=(), limit=16, flops=0, moved=0, alias=None):
    return pl.pallas_call(
        kernel,
        in_specs=ins,
        out_specs=outs,
        out_shape=shapes,
        scratch_shapes=scratch,
        compiler_params=pltpu.CompilerParams(vmem_limit_bytes=limit << 20),
        cost_estimate=pl.CostEstimate(flops=flops, bytes_accessed=moved, transcendentals=0),
        input_output_aliases=alias or {},
    )


def shards(grids, first_level, coeffs, slot_map):
    rows = grids[0]
    width = rows.shape[1]
    half = width // 2
    chunk = half // MEMBERS
    slabs = lax.axis_size("slab")
    members = lax.axis_size("grp")
    swap = [(i, i ^ 1) for i in range(members)]
    forth, back = (jnp.asarray(table, jnp.bfloat16) for table in row_tables())

    def to_previous(values, turn):
        pairs = [
            (g * slabs + s, (g ^ turn) * slabs + (s - 1) % slabs)
            for g in range(members)
            for s in range(slabs)
        ]
        return lax.ppermute(values, ("grp", "slab"), pairs)

    def through_tile(pieces):
        turned = lambda turn: [(tile[i], tile[i ^ turn]) for tile in TILES for i in range(MEMBERS)]
        far = {}
        for turn in (3, 2, 1):
            far[turn] = lax.ppermute(pieces[turn], "grp", turned(turn))
        return [pieces[0], far[1], far[2], far[3]]

    entry, own_plane, other_plane = call(
        entry_kernel, [VMEM], [VMEM] * 3,
        [f32(ROWS + 8, half), f32(PLANE, half), f32(PLANE, half)],
    )(rows)
    other_next = to_previous(other_plane, 1)
    own_next = to_previous(own_plane, 0)
    entry = call(stamp_kernel, [SMEM, SMEM, VMEM], VMEM, f32(ROWS + 8, half), alias={2: 0})(first_level, coeffs, entry)
    other = lax.ppermute(entry, "grp", swap)

    def surplus(*turns):
        return call(
            functools.partial(forth_kernel, turns), [SMEM, SMEM] + [VMEM] * 5, [VMEM] * len(turns),
            [f32(SENT, chunk)] * len(turns), flops=10**9,
        )(first_level, coeffs, forth, rows, own_next, other, other_next)

    sent = surplus(1, 2, 3)
    (stays,) = surplus(0)
    meta = call(meta_kernel, [VMEM], VMEM, f32(8, LANES))(other)
    got = through_tile([stays, *sent])

    parts = call(add_kernel, [VMEM] * MEMBERS, VMEM, f32(MEMBERS, TABLE, LANES), flops=10**8)(*got)
    for groups in (LINES, OTHER_LINES):
        parts = exchange(parts, groups)
        parts = call(total_kernel, [VMEM], VMEM, f32(MEMBERS, TABLE, LANES), flops=10**8)(parts)
    table = exchange(parts, LINES)
    picked = call(
        pick_kernel, [VMEM] * (MEMBERS + 1), [VMEM] * MEMBERS, [f32(FLAGS, chunk)] * MEMBERS, flops=10**8
    )(table, *got)
    final = through_tile(picked)

    other_out = call(
        other_back_kernel, [SMEM] + [VMEM] * (MEMBERS + 2), VMEM, f32(ROWS, half), flops=10**9
    )(first_level, meta, back, *final)
    swapped = lax.ppermute(other_out, "grp", swap)
    out = call(
        own_back_kernel, [SMEM] + [VMEM] * (MEMBERS + 2), HBM, f32(ROWS, width),
        (pltpu.VMEM((2 * MEMBERS, ROWS, chunk // 2), jnp.float32), DMA((2 * MEMBERS,))), flops=10**9,
    )(first_level, meta, back, *final)
    out = call(place_kernel, [VMEM, HBM], HBM, f32(ROWS, width), (DMA((ROWS // SHARE,)),), alias={1: 0})(swapped, out)
    return out[None]


def solution(mesh):
    in_specs = (P("grp", "slab", None), P("grp"), P("grp"), P("grp", "slab"))
    out_specs = P("grp", "slab", None)
    return jax.shard_map(shards, mesh=mesh, in_specs=in_specs, out_specs=out_specs, check_vma=False)
```

```python
import functools

import jax
import jax.numpy as jnp
import numpy as np
from jax import lax
from jax.experimental import pallas as pl
from jax.experimental.pallas import tpu as pltpu
from jax.sharding import PartitionSpec as P

LEVEL_SUM = 9
LOW_LEVEL = 6
NY = 8
NZ = 8
MEMBERS = 4
ROWS = 128
PLANE = 8
BLOCK = 32
SLOTS = 7
THERE = SLOTS * BLOCK
FLAGS = THERE + PLANE
SENT = FLAGS + 8
ENTRY = 2 * (ROWS + PLANE)
TABLE = 8 * BLOCK + PLANE
LANES = 128
SHARE = 16


def slots_of(levels):
    six, seven, eight = (level in levels for level in (6, 7, 8))
    third = 3 if six else (5 if seven else None)
    fifth = 6 if eight else (5 if six and seven else None)
    return (0, 1, 2, third, 4, fifth, 7)


def place_of(x, y):
    if x % 4 == 0 and y % 4 == 0:
        return (x // 4) * 2 + y // 4
    if x % 4 == 0 and y % 2 == 0:
        return 32 + (x // 4) * 2 + y // 4
    if x % 4 == 2 and y % 4 == 0:
        return 64 + (x // 4) * 2 + y // 4
    if x % 4 == 0:
        return 96 + (x // 4) * 4 + y // 2
    if x % 4 == 2:
        return 160 + (x // 4) * 2 + y // 4
    return 192 + (x // 2) * 2 + y // 4


def hier_line(n):
    h = np.zeros((n, n), np.float32)
    for j in range(n):
        h[j, j] += 1.0
        if j:
            s = j & -j
            h[j, j - s] -= 0.5
            h[j, (j + s) % n] -= 0.5
    return h


def dehier_line(n):
    e = np.zeros((n, n), np.float32)
    e[:, 0] = 1.0
    for k in range(1, n):
        for j in range(n):
            d = min(abs(j - k), n - abs(j - k))
            e[j, k] = max(0.0, 1.0 - d / (k & -k))
    return e


def one_grid(level, slots):
    n = 1 << (LEVEL_SUM - level)
    span = ROWS // n
    hy, ey = hier_line(n), dehier_line(n)
    forth = np.zeros((SENT, ROWS + PLANE), np.float32)
    back = np.zeros((ROWS, FLAGS), np.float32)
    for i in range(span):
        for y in range(n):
            t = place_of(i * 64 // span, y * 8 // n)
            m = BLOCK * slots.index(t // BLOCK) + t % BLOCK
            s = i & -i
            steps = [(i, 1.0)] + ([(i - s, -0.5), (i + s, -0.5)] if i else [])
            for j, w in steps:
                forth[m, j * n : j * n + n] += w * hy[y]
            for j in range(span):
                w = max(0.0, 1.0 - abs(j - i) / s) if i else 1.0 - j / span
                back[j * n : j * n + n, m] += w * ey[:, y]
    for y in range(n):
        t = THERE + y * 8 // n
        forth[t, ROWS : ROWS + n] += hy[y]
        for j in range(span):
            back[j * n : j * n + n, t] += j / span * ey[:, y]
    return forth, back


@functools.cache
def row_tables():
    forth, back = [], []
    for own in (6, 7, 8):
        for other in (6, 7, 8):
            slots = slots_of((own, other))
            mine, theirs = one_grid(own, slots), one_grid(other, slots)
            forth.append(np.concatenate([mine[0], theirs[0]], axis=1))
            back.append(mine[1])
    return np.stack(forth), np.stack(back)


def two_part_dot(table, values):
    high = values.astype(jnp.bfloat16)
    low = (values - high.astype(jnp.float32)).astype(jnp.bfloat16)
    dot = functools.partial(jnp.dot, preferred_element_type=jnp.float32)
    return dot(table, high) + dot(table, low)


def number_in(ref, row):
    return jnp.max(ref[row : row + 1, :LANES])


def core_here():
    return lax.axis_index("grp") % 2


def piece_here(turn):
    me = lax.axis_index("grp")
    core, z, y = me % 2, me // 2 % NZ, me // (2 * NZ)
    return ((y + core) % 2 * 2 + (z + core) % 2) ^ turn


def half_of(ref, core, rows=slice(None)):
    width = ref.shape[1] // 2
    return ref.at[rows, pl.ds(pl.multiple_of(core * width, LANES), width)]


def lead_kernel(out_ref):
    out_ref[...] = lax.broadcasted_iota(jnp.int32, out_ref.shape, 0)


def numbers_kernel(level_ref, coeff_ref, line_ref, out_ref):
    out_ref[...] = jnp.where(line_ref[...] == 0, level_ref[0], coeff_ref[0]).astype(jnp.float32)


def entry_kernel(numbers_ref, rows_ref, out_ref, own_plane_ref, other_plane_ref):
    core = core_here()
    half = out_ref.shape[1]
    mine = pl.ds(pl.multiple_of(core * half, LANES), half)
    theirs = pl.ds(pl.multiple_of((1 - core) * half, LANES), half)
    own_plane_ref[...] = rows_ref[:PLANE, mine]
    other_plane_ref[...] = rows_ref[:PLANE, theirs]
    out_ref[:ROWS, :] = rows_ref[:, theirs]
    out_ref[ROWS:, :] = jnp.concatenate([numbers_ref[...]] * (half // LANES), axis=1)


def forth_kernel(turns, level_ref, coeff_ref, table_ref, rows_ref, own_next_ref, other_ref, other_next_ref, *out_refs):
    own_level = level_ref[0]
    other_level = number_in(other_ref, ROWS).astype(jnp.int32)
    which = (own_level - LOW_LEVEL) * 3 + other_level - LOW_LEVEL
    chunk = out_refs[0].shape[1]
    lane = lax.broadcasted_iota(jnp.int32, (1, ENTRY), 1)
    scale = jnp.where(lane < ENTRY // 2, coeff_ref[0].astype(jnp.float32), number_in(other_ref, ROWS + 1))
    table = (table_ref[which].astype(jnp.float32) * scale).astype(jnp.bfloat16)
    six = jnp.logical_or(own_level == 6, other_level == 6).astype(jnp.float32)
    eight = jnp.logical_or(own_level == 8, other_level == 8).astype(jnp.float32)
    width = chunk // 2
    line = lax.broadcasted_iota(jnp.int32, (SENT - FLAGS, width), 0)
    flags = jnp.where(line == 0, six, eight)
    first = core_here() * MEMBERS * chunk
    for turn, out_ref in zip(turns, out_refs):
        for h in range(2):
            here = slice(h * width, (h + 1) * width)
            low = piece_here(turn) * chunk + h * width
            span = pl.ds(pl.multiple_of(low, LANES), width)
            own = rows_ref[:, pl.ds(pl.multiple_of(first + low, LANES), width)]
            values = jnp.concatenate(
                [own, own_next_ref[:, span], other_ref[:ROWS, span], other_next_ref[:, span]], axis=0
            )
            out_ref[:, here] = two_part_dot(table, values)
            out_ref[FLAGS:SENT, here] = flags


def meta_kernel(other_ref, meta_ref):
    meta_ref[...] = other_ref[ROWS:, :LANES]


def add_kernel(*refs):
    *got_refs, out_ref = refs
    for j in range(MEMBERS):
        lanes = slice(j * LANES, (j + 1) * LANES)
        six = [ref[FLAGS : FLAGS + 1, lanes] == 1.0 for ref in got_refs]
        eight = [ref[FLAGS + 1 : FLAGS + 2, lanes] == 1.0 for ref in got_refs]
        slot = lambda k, i: got_refs[k][BLOCK * i : BLOCK * (i + 1), lanes]
        terms = (
            lambda k: slot(k, 0),
            lambda k: slot(k, 1),
            lambda k: slot(k, 2),
            lambda k: jnp.where(six[k], slot(k, 3), 0.0),
            lambda k: slot(k, 4),
            lambda k: jnp.where(six[k], jnp.where(eight[k], 0.0, slot(k, 5)), slot(k, 3)),
            lambda k: jnp.where(eight[k], slot(k, 5), 0.0),
            lambda k: slot(k, 6),
            lambda k: got_refs[k][THERE:FLAGS, lanes],
        )
        for block, term in enumerate(terms):
            total = term(0)
            for k in range(1, MEMBERS):
                total = total + term(k)
            out_ref[j, BLOCK * block : BLOCK * block + total.shape[0], :] = total


def total_kernel(got_ref, out_ref):
    total = got_ref[0]
    for k in range(1, MEMBERS):
        total = total + got_ref[k]
    for k in range(MEMBERS):
        out_ref[k] = total


def pick_kernel(table_ref, *refs):
    for got_ref, out_ref in zip(refs[:MEMBERS], refs[MEMBERS:]):
        for j in range(MEMBERS):
            lanes = slice(j * LANES, (j + 1) * LANES)
            block = lambda i: table_ref[j, BLOCK * i : BLOCK * (i + 1), :]
            six = got_ref[FLAGS : FLAGS + 1, lanes] == 1.0
            eight = got_ref[FLAGS + 1 : FLAGS + 2, lanes] == 1.0
            out_ref[0:32, lanes] = block(0)
            out_ref[32:64, lanes] = block(1)
            out_ref[64:96, lanes] = block(2)
            out_ref[96:128, lanes] = jnp.where(six, block(3), block(5))
            out_ref[128:160, lanes] = block(4)
            out_ref[160:192, lanes] = jnp.where(eight, block(6), block(5))
            out_ref[192:224, lanes] = block(7)
            out_ref[THERE:FLAGS, lanes] = table_ref[j, 8 * BLOCK : TABLE, :]


def levels_in(level_ref, meta_ref):
    return level_ref[0] - LOW_LEVEL, number_in(meta_ref, 0).astype(jnp.int32) - LOW_LEVEL


def pieces(refs):
    for turn, ref in enumerate(refs):
        chunk = ref.shape[1]
        for h in range(2):
            width = chunk // 2
            yield piece_here(turn) * chunk + h * width, ref[:, h * width : (h + 1) * width]


def other_back_kernel(level_ref, meta_ref, table_ref, *refs):
    *got_refs, out_ref = refs
    own, other = levels_in(level_ref, meta_ref)
    table = table_ref[other * 3 + own]
    for low, values in pieces(got_refs):
        out_ref[:, pl.ds(pl.multiple_of(low, LANES), values.shape[1])] = two_part_dot(table, values)


def own_back_kernel(level_ref, meta_ref, table_ref, *refs):
    *got_refs, out_ref, done_ref, sems = refs
    own, other = levels_in(level_ref, meta_ref)
    table = table_ref[own * 3 + other]
    first = core_here() * (out_ref.shape[1] // 2)
    copies = []
    for i, (low, values) in enumerate(pieces(got_refs)):
        width = values.shape[1]
        done_ref[i] = two_part_dot(table, values)
        start = pl.multiple_of(first + low, LANES)
        copy = pltpu.make_async_copy(done_ref.at[i], out_ref.at[:, pl.ds(start, width)], sems.at[i])
        copy.start()
        copies.append(copy)
    for copy in copies:
        copy.wait()


def place_kernel(values_ref, filled_ref, out_ref, sems):
    copies = []
    for i in range(ROWS // SHARE):
        part = slice(i * SHARE, (i + 1) * SHARE)
        to = half_of(out_ref, 1 - core_here(), part)
        copies.append(pltpu.make_async_copy(values_ref.at[part], to, sems.at[i]))
    for copy in copies:
        copy.start()
    for copy in copies:
        copy.wait()


def member(y, z, core):
    return (y % NY * NZ + z % NZ) * 2 + core


TILES = [
    [member(2 * a + i + core, 2 * b + j + core, core) for i in (0, 1) for j in (0, 1)]
    for core in (0, 1)
    for a in range(NY // 2)
    for b in range(NZ // 2)
]
ALONG_Y = [[[member(2 * a + i, z, core) for a in range(NY // 2)] for i in (0, 1) for z in range(NZ)] for core in (0, 1)]
ALONG_Z = [[[member(y, 2 * b + j, core) for b in range(NZ // 2)] for j in (0, 1) for y in range(NY)] for core in (0, 1)]
LINES = ALONG_Z[0] + ALONG_Y[1]
OTHER_LINES = ALONG_Y[0] + ALONG_Z[1]
VMEM = pl.BlockSpec(memory_space=pltpu.VMEM)
SMEM = pl.BlockSpec(memory_space=pltpu.SMEM)
HBM = pl.BlockSpec(memory_space=pltpu.HBM)
DMA = pltpu.SemaphoreType.DMA


def exchange(values, groups):
    return lax.all_to_all(values, "grp", 0, 0, axis_index_groups=groups, tiled=True)


def f32(*shape):
    return jax.ShapeDtypeStruct(shape, jnp.float32)


def call(kernel, ins, outs, shapes, scratch=(), limit=16, flops=0, moved=0, alias=None):
    return pl.pallas_call(
        kernel,
        in_specs=ins,
        out_specs=outs,
        out_shape=shapes,
        scratch_shapes=scratch,
        compiler_params=pltpu.CompilerParams(vmem_limit_bytes=limit << 20),
        cost_estimate=pl.CostEstimate(flops=flops, bytes_accessed=moved, transcendentals=0),
        input_output_aliases=alias or {},
    )


def shards(grids, first_level, coeffs, slot_map):
    rows = grids[0]
    width = rows.shape[1]
    half = width // 2
    chunk = half // MEMBERS
    slabs = lax.axis_size("slab")
    members = lax.axis_size("grp")
    swap = [(i, i ^ 1) for i in range(members)]
    forth, back = (jnp.asarray(table, jnp.bfloat16) for table in row_tables())

    def to_previous(values, turn):
        pairs = [
            (g * slabs + s, (g ^ turn) * slabs + (s - 1) % slabs)
            for g in range(members)
            for s in range(slabs)
        ]
        return lax.ppermute(values, ("grp", "slab"), pairs)

    def through_tile(pieces):
        turned = lambda turn: [(tile[i], tile[i ^ turn]) for tile in TILES for i in range(MEMBERS)]
        far = {}
        for turn in (3, 2, 1):
            far[turn] = lax.ppermute(pieces[turn], "grp", turned(turn))
        return [pieces[0], far[1], far[2], far[3]]

    line = call(lead_kernel, [], VMEM, jax.ShapeDtypeStruct((8, LANES), jnp.int32), flops=2*10**9)()
    numbers = call(numbers_kernel, [SMEM, SMEM, VMEM], VMEM, f32(8, LANES))(first_level, coeffs, line)
    entry, own_plane, other_plane = call(
        entry_kernel, [VMEM] * 2, [VMEM] * 3,
        [f32(ROWS + 8, half), f32(PLANE, half), f32(PLANE, half)],
    )(numbers, rows)
    other_next = to_previous(other_plane, 1)
    own_next = to_previous(own_plane, 0)
    other = lax.ppermute(entry, "grp", swap)

    def surplus(*turns):
        return call(
            functools.partial(forth_kernel, turns), [SMEM, SMEM] + [VMEM] * 5, [VMEM] * len(turns),
            [f32(SENT, chunk)] * len(turns), flops=10**9,
        )(first_level, coeffs, forth, rows, own_next, other, other_next)

    sent = surplus(1, 2, 3)
    (stays,) = surplus(0)
    meta = call(meta_kernel, [VMEM], VMEM, f32(8, LANES))(other)
    got = through_tile([stays, *sent])

    parts = call(add_kernel, [VMEM] * MEMBERS, VMEM, f32(MEMBERS, TABLE, LANES), flops=10**8)(*got)
    for groups in (LINES, OTHER_LINES):
        parts = exchange(parts, groups)
        parts = call(total_kernel, [VMEM], VMEM, f32(MEMBERS, TABLE, LANES), flops=10**8)(parts)
    table = exchange(parts, LINES)
    picked = call(
        pick_kernel, [VMEM] * (MEMBERS + 1), [VMEM] * MEMBERS, [f32(FLAGS, chunk)] * MEMBERS, flops=10**8
    )(table, *got)
    final = through_tile(picked)

    other_out = call(
        other_back_kernel, [SMEM] + [VMEM] * (MEMBERS + 2), VMEM, f32(ROWS, half), flops=10**9
    )(first_level, meta, back, *final)
    swapped = lax.ppermute(other_out, "grp", swap)
    out = call(
        own_back_kernel, [SMEM] + [VMEM] * (MEMBERS + 2), HBM, f32(ROWS, width),
        (pltpu.VMEM((2 * MEMBERS, ROWS, chunk // 2), jnp.float32), DMA((2 * MEMBERS,))), flops=10**9,
    )(first_level, meta, back, *final)
    out = call(place_kernel, [VMEM, HBM], HBM, f32(ROWS, width), (DMA((ROWS // SHARE,)),), alias={1: 0})(swapped, out)
    return out[None]


def solution(mesh):
    in_specs = (P("grp", "slab", None), P("grp"), P("grp"), P("grp", "slab"))
    out_specs = P("grp", "slab", None)
    return jax.shard_map(shards, mesh=mesh, in_specs=in_specs, out_specs=out_specs, check_vma=False)
```

```python
import functools

import jax
import jax.numpy as jnp
import numpy as np
from jax import lax
from jax.experimental import pallas as pl
from jax.experimental.pallas import tpu as pltpu
from jax.sharding import PartitionSpec as P

LEVEL_SUM = 9
LOW_LEVEL = 6
NY = 8
NZ = 8
MEMBERS = 4
ROWS = 128
PLANE = 8
BLOCK = 32
SLOTS = 7
THERE = SLOTS * BLOCK
FLAGS = THERE + PLANE
SENT = FLAGS + 8
ENTRY = 2 * (ROWS + PLANE)
TABLE = 8 * BLOCK + PLANE
LANES = 128


def slots_of(levels):
    six, seven, eight = (level in levels for level in (6, 7, 8))
    third = 3 if six else (5 if seven else None)
    fifth = 6 if eight else (5 if six and seven else None)
    return (0, 1, 2, third, 4, fifth, 7)


def place_of(x, y):
    if x % 4 == 0 and y % 4 == 0:
        return (x // 4) * 2 + y // 4
    if x % 4 == 0 and y % 2 == 0:
        return 32 + (x // 4) * 2 + y // 4
    if x % 4 == 2 and y % 4 == 0:
        return 64 + (x // 4) * 2 + y // 4
    if x % 4 == 0:
        return 96 + (x // 4) * 4 + y // 2
    if x % 4 == 2:
        return 160 + (x // 4) * 2 + y // 4
    return 192 + (x // 2) * 2 + y // 4


def hier_line(n):
    h = np.zeros((n, n), np.float32)
    for j in range(n):
        h[j, j] += 1.0
        if j:
            s = j & -j
            h[j, j - s] -= 0.5
            h[j, (j + s) % n] -= 0.5
    return h


def dehier_line(n):
    e = np.zeros((n, n), np.float32)
    e[:, 0] = 1.0
    for k in range(1, n):
        for j in range(n):
            d = min(abs(j - k), n - abs(j - k))
            e[j, k] = max(0.0, 1.0 - d / (k & -k))
    return e


def one_grid(level, slots):
    n = 1 << (LEVEL_SUM - level)
    span = ROWS // n
    hy, ey = hier_line(n), dehier_line(n)
    forth = np.zeros((SENT, ROWS + PLANE), np.float32)
    back = np.zeros((ROWS, FLAGS), np.float32)
    for i in range(span):
        for y in range(n):
            t = place_of(i * 64 // span, y * 8 // n)
            m = BLOCK * slots.index(t // BLOCK) + t % BLOCK
            s = i & -i
            steps = [(i, 1.0)] + ([(i - s, -0.5), (i + s, -0.5)] if i else [])
            for j, w in steps:
                forth[m, j * n : j * n + n] += w * hy[y]
            for j in range(span):
                w = max(0.0, 1.0 - abs(j - i) / s) if i else 1.0 - j / span
                back[j * n : j * n + n, m] += w * ey[:, y]
    for y in range(n):
        t = THERE + y * 8 // n
        forth[t, ROWS : ROWS + n] += hy[y]
        for j in range(span):
            back[j * n : j * n + n, t] += j / span * ey[:, y]
    return forth, back


@functools.cache
def row_tables():
    forth, back = [], []
    for own in (6, 7, 8):
        for other in (6, 7, 8):
            slots = slots_of((own, other))
            mine, theirs = one_grid(own, slots), one_grid(other, slots)
            forth.append(np.concatenate([mine[0], theirs[0]], axis=1))
            back.append(mine[1])
    return np.stack(forth), np.stack(back)


def two_part_dot(table, values):
    high = values.astype(jnp.bfloat16)
    low = (values - high.astype(jnp.float32)).astype(jnp.bfloat16)
    dot = functools.partial(jnp.dot, preferred_element_type=jnp.float32)
    return dot(table, high) + dot(table, low)


def number_in(ref, row):
    return jnp.max(ref[row : row + 1, :LANES])


def core_here():
    return lax.axis_index("grp") % 2


def piece_here(turn):
    me = lax.axis_index("grp")
    core, z, y = me % 2, me // 2 % NZ, me // (2 * NZ)
    return ((y + core) % 2 * 2 + (z + core) % 2) ^ turn


def lead_kernel(out_ref):
    out_ref[...] = lax.broadcasted_iota(jnp.int32, out_ref.shape, 0)


def numbers_kernel(level_ref, coeff_ref, line_ref, out_ref):
    out_ref[...] = jnp.where(line_ref[...] == 0, level_ref[0], coeff_ref[0]).astype(jnp.float32)


def entry_kernel(numbers_ref, rows_ref, out_ref, own_plane_ref, other_plane_ref):
    core = core_here()
    half = out_ref.shape[1]
    mine = pl.ds(pl.multiple_of(core * half, LANES), half)
    theirs = pl.ds(pl.multiple_of((1 - core) * half, LANES), half)
    own_plane_ref[...] = rows_ref[:PLANE, mine]
    other_plane_ref[...] = rows_ref[:PLANE, theirs]
    out_ref[:ROWS, :] = rows_ref[:, theirs]
    out_ref[ROWS:, :] = jnp.concatenate([numbers_ref[...]] * (half // LANES), axis=1)


def forth_kernel(turns, level_ref, coeff_ref, table_ref, rows_ref, own_next_ref, other_ref, other_next_ref, *out_refs):
    own_level = level_ref[0]
    other_level = number_in(other_ref, ROWS).astype(jnp.int32)
    which = (own_level - LOW_LEVEL) * 3 + other_level - LOW_LEVEL
    chunk = out_refs[0].shape[1]
    lane = lax.broadcasted_iota(jnp.int32, (1, ENTRY), 1)
    scale = jnp.where(lane < ENTRY // 2, coeff_ref[0].astype(jnp.float32), number_in(other_ref, ROWS + 1))
    table = (table_ref[which].astype(jnp.float32) * scale).astype(jnp.bfloat16)
    six = jnp.logical_or(own_level == 6, other_level == 6).astype(jnp.float32)
    eight = jnp.logical_or(own_level == 8, other_level == 8).astype(jnp.float32)
    width = chunk // 2
    line = lax.broadcasted_iota(jnp.int32, (SENT - FLAGS, width), 0)
    flags = jnp.where(line == 0, six, eight)
    first = core_here() * MEMBERS * chunk
    for turn, out_ref in zip(turns, out_refs):
        for h in range(2):
            here = slice(h * width, (h + 1) * width)
            low = piece_here(turn) * chunk + h * width
            span = pl.ds(pl.multiple_of(low, LANES), width)
            own = rows_ref[:, pl.ds(pl.multiple_of(first + low, LANES), width)]
            values = jnp.concatenate(
                [own, own_next_ref[:, span], other_ref[:ROWS, span], other_next_ref[:, span]], axis=0
            )
            out_ref[:, here] = two_part_dot(table, values)
            out_ref[FLAGS:SENT, here] = flags


def meta_kernel(other_ref, meta_ref):
    meta_ref[...] = other_ref[ROWS:, :LANES]


def add_kernel(*refs):
    *got_refs, out_ref = refs
    for j in range(MEMBERS):
        lanes = slice(j * LANES, (j + 1) * LANES)
        six = [ref[FLAGS : FLAGS + 1, lanes] == 1.0 for ref in got_refs]
        eight = [ref[FLAGS + 1 : FLAGS + 2, lanes] == 1.0 for ref in got_refs]
        slot = lambda k, i: got_refs[k][BLOCK * i : BLOCK * (i + 1), lanes]
        terms = (
            lambda k: slot(k, 0),
            lambda k: slot(k, 1),
            lambda k: slot(k, 2),
            lambda k: jnp.where(six[k], slot(k, 3), 0.0),
            lambda k: slot(k, 4),
            lambda k: jnp.where(six[k], jnp.where(eight[k], 0.0, slot(k, 5)), slot(k, 3)),
            lambda k: jnp.where(eight[k], slot(k, 5), 0.0),
            lambda k: slot(k, 6),
            lambda k: got_refs[k][THERE:FLAGS, lanes],
        )
        for block, term in enumerate(terms):
            total = term(0)
            for k in range(1, MEMBERS):
                total = total + term(k)
            out_ref[j, BLOCK * block : BLOCK * block + total.shape[0], :] = total


def total_kernel(got_ref, out_ref):
    total = got_ref[0]
    for k in range(1, MEMBERS):
        total = total + got_ref[k]
    for k in range(MEMBERS):
        out_ref[k] = total


def pick_kernel(table_ref, *refs):
    for got_ref, out_ref in zip(refs[:MEMBERS], refs[MEMBERS:]):
        for j in range(MEMBERS):
            lanes = slice(j * LANES, (j + 1) * LANES)
            block = lambda i: table_ref[j, BLOCK * i : BLOCK * (i + 1), :]
            six = got_ref[FLAGS : FLAGS + 1, lanes] == 1.0
            eight = got_ref[FLAGS + 1 : FLAGS + 2, lanes] == 1.0
            out_ref[0:32, lanes] = block(0)
            out_ref[32:64, lanes] = block(1)
            out_ref[64:96, lanes] = block(2)
            out_ref[96:128, lanes] = jnp.where(six, block(3), block(5))
            out_ref[128:160, lanes] = block(4)
            out_ref[160:192, lanes] = jnp.where(eight, block(6), block(5))
            out_ref[192:224, lanes] = block(7)
            out_ref[THERE:FLAGS, lanes] = table_ref[j, 8 * BLOCK : TABLE, :]


def levels_in(level_ref, meta_ref):
    return level_ref[0] - LOW_LEVEL, number_in(meta_ref, 0).astype(jnp.int32) - LOW_LEVEL


def pieces(ref):
    width = ref.shape[1] // 2
    for h in range(2):
        yield h * width, ref[:, h * width : (h + 1) * width]


def other_back_kernel(level_ref, meta_ref, table_ref, *refs):
    *got_refs, out_ref = refs
    own, other = levels_in(level_ref, meta_ref)
    table = table_ref[other * 3 + own]
    for i, ref in enumerate(got_refs):
        for low, values in pieces(ref):
            out_ref[i, :, low : low + values.shape[1]] = two_part_dot(table, values)


def own_back_kernel(turns, level_ref, meta_ref, table_ref, *refs):
    got_refs = refs[: len(turns)]
    out_ref, done_ref, sems = refs[-3:]
    own, other = levels_in(level_ref, meta_ref)
    table = table_ref[own * 3 + other]
    first = core_here() * (out_ref.shape[1] // 2)
    copies = []
    for turn, ref in zip(turns, got_refs):
        for low, values in pieces(ref):
            i, width = len(copies), values.shape[1]
            done_ref[i] = two_part_dot(table, values)
            start = pl.multiple_of(first + piece_here(turn) * ref.shape[1] + low, LANES)
            copy = pltpu.make_async_copy(done_ref.at[i], out_ref.at[:, pl.ds(start, width)], sems.at[i])
            copy.start()
            copies.append(copy)
    for copy in copies:
        copy.wait()


def place_kernel(turns, values_ref, filled_ref, out_ref, sems):
    first = (1 - core_here()) * (out_ref.shape[1] // 2)
    width = values_ref.shape[2]
    copies = []
    for i, turn in enumerate(turns):
        start = pl.multiple_of(first + (piece_here(turn) ^ 3) * width, LANES)
        copies.append(
            pltpu.make_async_copy(values_ref.at[i], out_ref.at[:, pl.ds(start, width)], sems.at[i])
        )
    for copy in copies:
        copy.start()
    for copy in copies:
        copy.wait()


def member(y, z, core):
    return (y % NY * NZ + z % NZ) * 2 + core


TILES = [
    [member(2 * a + i + core, 2 * b + j + core, core) for i in (0, 1) for j in (0, 1)]
    for core in (0, 1)
    for a in range(NY // 2)
    for b in range(NZ // 2)
]
ALONG_Y = [[[member(2 * a + i, z, core) for a in range(NY // 2)] for i in (0, 1) for z in range(NZ)] for core in (0, 1)]
ALONG_Z = [[[member(y, 2 * b + j, core) for b in range(NZ // 2)] for j in (0, 1) for y in range(NY)] for core in (0, 1)]
LINES = ALONG_Z[0] + ALONG_Y[1]
OTHER_LINES = ALONG_Y[0] + ALONG_Z[1]
VMEM = pl.BlockSpec(memory_space=pltpu.VMEM)
SMEM = pl.BlockSpec(memory_space=pltpu.SMEM)
HBM = pl.BlockSpec(memory_space=pltpu.HBM)
DMA = pltpu.SemaphoreType.DMA


def exchange(values, groups):
    return lax.all_to_all(values, "grp", 0, 0, axis_index_groups=groups, tiled=True)


def f32(*shape):
    return jax.ShapeDtypeStruct(shape, jnp.float32)


def call(kernel, ins, outs, shapes, scratch=(), limit=16, flops=0, moved=0, alias=None):
    return pl.pallas_call(
        kernel,
        in_specs=ins,
        out_specs=outs,
        out_shape=shapes,
        scratch_shapes=scratch,
        compiler_params=pltpu.CompilerParams(vmem_limit_bytes=limit << 20),
        cost_estimate=pl.CostEstimate(flops=flops, bytes_accessed=moved, transcendentals=0),
        input_output_aliases=alias or {},
    )


def shards(grids, first_level, coeffs, slot_map):
    rows = grids[0]
    width = rows.shape[1]
    half = width // 2
    chunk = half // MEMBERS
    slabs = lax.axis_size("slab")
    members = lax.axis_size("grp")
    swap = [(i, i ^ 1) for i in range(members)]
    forth, back = (jnp.asarray(table, jnp.bfloat16) for table in row_tables())

    def to_previous(values, turn):
        pairs = [
            (g * slabs + s, (g ^ turn) * slabs + (s - 1) % slabs)
            for g in range(members)
            for s in range(slabs)
        ]
        return lax.ppermute(values, ("grp", "slab"), pairs)

    def through_tile(pieces):
        turned = lambda turn: [(tile[i], tile[i ^ turn]) for tile in TILES for i in range(MEMBERS)]
        far = {}
        for turn in (3, 2, 1):
            far[turn] = lax.ppermute(pieces[turn], "grp", turned(turn))
        return [pieces[0], far[1], far[2], far[3]]

    line = call(lead_kernel, [], VMEM, jax.ShapeDtypeStruct((8, LANES), jnp.int32), flops=2*10**9)()
    numbers = call(numbers_kernel, [SMEM, SMEM, VMEM], VMEM, f32(8, LANES))(first_level, coeffs, line)
    entry, own_plane, other_plane = call(
        entry_kernel, [VMEM] * 2, [VMEM] * 3,
        [f32(ROWS + 8, half), f32(PLANE, half), f32(PLANE, half)],
    )(numbers, rows)
    other_next = to_previous(other_plane, 1)
    own_next = to_previous(own_plane, 0)
    other = lax.ppermute(entry, "grp", swap)

    def surplus(*turns):
        return call(
            functools.partial(forth_kernel, turns), [SMEM, SMEM] + [VMEM] * 5, [VMEM] * len(turns),
            [f32(SENT, chunk)] * len(turns), flops=10**9,
        )(first_level, coeffs, forth, rows, own_next, other, other_next)

    sent = surplus(1, 2, 3)
    (stays,) = surplus(0)
    meta = call(meta_kernel, [VMEM], VMEM, f32(8, LANES))(other)
    got = through_tile([stays, *sent])

    parts = call(add_kernel, [VMEM] * MEMBERS, VMEM, f32(MEMBERS, TABLE, LANES), flops=10**8)(*got)
    for groups in (LINES, OTHER_LINES):
        parts = exchange(parts, groups)
        parts = call(total_kernel, [VMEM], VMEM, f32(MEMBERS, TABLE, LANES), flops=10**8)(parts)
    table = exchange(parts, LINES)
    picked = call(
        pick_kernel, [VMEM] * (MEMBERS + 1), [VMEM] * MEMBERS, [f32(FLAGS, chunk)] * MEMBERS, flops=10**8
    )(table, *got)
    final = through_tile(picked)

    def other_rows(turns):
        return call(
            other_back_kernel, [SMEM] + [VMEM] * (2 + len(turns)), VMEM,
            f32(len(turns), ROWS, chunk), flops=10**9,
        )(first_level, meta, back, *[final[turn] for turn in turns])

    def own_rows(turns, *filled):
        parts = 2 * len(turns)
        return call(
            functools.partial(own_back_kernel, turns),
            [SMEM] + [VMEM] * (2 + len(turns)) + [HBM] * len(filled), HBM, f32(ROWS, width),
            (pltpu.VMEM((parts, ROWS, chunk // 2), jnp.float32), DMA((parts,))), flops=10**9,
            alias={3 + len(turns): 0} if filled else None,
        )(first_level, meta, back, *[final[turn] for turn in turns], *filled)

    def place(turns, values, filled):
        return call(
            functools.partial(place_kernel, turns), [VMEM, HBM], HBM, f32(ROWS, width),
            (DMA((len(turns),)),), alias={1: 0}, flops=10**8,
        )(values, filled)

    early, late = (0, 3), (2, 1)
    other_early = other_rows(early)
    swapped_early = lax.ppermute(other_early, "grp", swap)
    out = own_rows(early)
    other_late = other_rows(late)
    swapped_late = lax.ppermute(other_late, "grp", swap)
    out = place(early, swapped_early, out)
    out = own_rows(late, out)
    out = place(late, swapped_late, out)
    return out[None]


def solution(mesh):
    in_specs = (P("grp", "slab", None), P("grp"), P("grp"), P("grp", "slab"))
    out_specs = P("grp", "slab", None)
    return jax.shard_map(shards, mesh=mesh, in_specs=in_specs, out_specs=out_specs, check_vma=False)
```

```python
import functools

import jax
import jax.numpy as jnp
import numpy as np
from jax import lax
from jax.experimental import pallas as pl
from jax.experimental.pallas import tpu as pltpu
from jax.sharding import PartitionSpec as P

LEVEL_SUM = 9
LOW_LEVEL = 6
NY = 8
NZ = 8
MEMBERS = 4
ROWS = 128
PLANE = 8
BLOCK = 32
SLOTS = 7
THERE = SLOTS * BLOCK
FLAGS = THERE + PLANE
SENT = FLAGS + 8
ENTRY = 2 * (ROWS + PLANE)
TABLE = 8 * BLOCK + PLANE
LANES = 128


def slots_of(levels):
    six, seven, eight = (level in levels for level in (6, 7, 8))
    third = 3 if six else (5 if seven else None)
    fifth = 6 if eight else (5 if six and seven else None)
    return (0, 1, 2, third, 4, fifth, 7)


def place_of(x, y):
    if x % 4 == 0 and y % 4 == 0:
        return (x // 4) * 2 + y // 4
    if x % 4 == 0 and y % 2 == 0:
        return 32 + (x // 4) * 2 + y // 4
    if x % 4 == 2 and y % 4 == 0:
        return 64 + (x // 4) * 2 + y // 4
    if x % 4 == 0:
        return 96 + (x // 4) * 4 + y // 2
    if x % 4 == 2:
        return 160 + (x // 4) * 2 + y // 4
    return 192 + (x // 2) * 2 + y // 4


def hier_line(n):
    h = np.zeros((n, n), np.float32)
    for j in range(n):
        h[j, j] += 1.0
        if j:
            s = j & -j
            h[j, j - s] -= 0.5
            h[j, (j + s) % n] -= 0.5
    return h


def dehier_line(n):
    e = np.zeros((n, n), np.float32)
    e[:, 0] = 1.0
    for k in range(1, n):
        for j in range(n):
            d = min(abs(j - k), n - abs(j - k))
            e[j, k] = max(0.0, 1.0 - d / (k & -k))
    return e


def one_grid(level, slots):
    n = 1 << (LEVEL_SUM - level)
    span = ROWS // n
    hy, ey = hier_line(n), dehier_line(n)
    forth = np.zeros((SENT, ROWS + PLANE), np.float32)
    back = np.zeros((ROWS, FLAGS), np.float32)
    for i in range(span):
        for y in range(n):
            t = place_of(i * 64 // span, y * 8 // n)
            m = BLOCK * slots.index(t // BLOCK) + t % BLOCK
            s = i & -i
            steps = [(i, 1.0)] + ([(i - s, -0.5), (i + s, -0.5)] if i else [])
            for j, w in steps:
                forth[m, j * n : j * n + n] += w * hy[y]
            for j in range(span):
                w = max(0.0, 1.0 - abs(j - i) / s) if i else 1.0 - j / span
                back[j * n : j * n + n, m] += w * ey[:, y]
    for y in range(n):
        t = THERE + y * 8 // n
        forth[t, ROWS : ROWS + n] += hy[y]
        for j in range(span):
            back[j * n : j * n + n, t] += j / span * ey[:, y]
    return forth, back


@functools.cache
def row_tables():
    forth, back = [], []
    for own in (6, 7, 8):
        for other in (6, 7, 8):
            slots = slots_of((own, other))
            mine, theirs = one_grid(own, slots), one_grid(other, slots)
            forth.append(np.concatenate([mine[0], theirs[0]], axis=1))
            back.append(mine[1])
    return np.stack(forth), np.stack(back)


def two_part_dot(table, values):
    high = values.astype(jnp.bfloat16)
    low = (values - high.astype(jnp.float32)).astype(jnp.bfloat16)
    dot = functools.partial(jnp.dot, preferred_element_type=jnp.float32)
    return dot(table, high) + dot(table, low)


def number_in(ref, row):
    return jnp.max(ref[row : row + 1, :LANES])


def core_here():
    return lax.axis_index("grp") % 2


def piece_here(turn):
    me = lax.axis_index("grp")
    core, z, y = me % 2, me // 2 % NZ, me // (2 * NZ)
    return ((y + core) % 2 * 2 + (z + core) % 2) ^ turn


def lead_kernel(out_ref):
    out_ref[...] = lax.broadcasted_iota(jnp.int32, out_ref.shape, 0)


def numbers_kernel(level_ref, coeff_ref, line_ref, out_ref):
    out_ref[...] = jnp.where(line_ref[...] == 0, level_ref[0], coeff_ref[0]).astype(jnp.float32)


def entry_kernel(numbers_ref, rows_ref, out_ref, own_plane_ref, other_plane_ref):
    core = core_here()
    half = out_ref.shape[1]
    mine = pl.ds(pl.multiple_of(core * half, LANES), half)
    theirs = pl.ds(pl.multiple_of((1 - core) * half, LANES), half)
    own_plane_ref[...] = rows_ref[:PLANE, mine]
    other_plane_ref[...] = rows_ref[:PLANE, theirs]
    out_ref[:ROWS, :] = rows_ref[:, theirs]
    out_ref[ROWS:, :] = jnp.concatenate([numbers_ref[...]] * (half // LANES), axis=1)


def forth_kernel(turns, level_ref, coeff_ref, table_ref, rows_ref, own_next_ref, other_ref, other_next_ref, *out_refs):
    own_level = level_ref[0]
    other_level = number_in(other_ref, ROWS).astype(jnp.int32)
    which = (own_level - LOW_LEVEL) * 3 + other_level - LOW_LEVEL
    chunk = out_refs[0].shape[1]
    lane = lax.broadcasted_iota(jnp.int32, (1, ENTRY), 1)
    scale = jnp.where(lane < ENTRY // 2, coeff_ref[0].astype(jnp.float32), number_in(other_ref, ROWS + 1))
    table = (table_ref[which].astype(jnp.float32) * scale).astype(jnp.bfloat16)
    six = jnp.logical_or(own_level == 6, other_level == 6).astype(jnp.float32)
    eight = jnp.logical_or(own_level == 8, other_level == 8).astype(jnp.float32)
    width = chunk // 2
    line = lax.broadcasted_iota(jnp.int32, (SENT - FLAGS, width), 0)
    flags = jnp.where(line == 0, six, eight)
    first = core_here() * MEMBERS * chunk
    for turn, out_ref in zip(turns, out_refs):
        for h in range(2):
            here = slice(h * width, (h + 1) * width)
            low = piece_here(turn) * chunk + h * width
            span = pl.ds(pl.multiple_of(low, LANES), width)
            own = rows_ref[:, pl.ds(pl.multiple_of(first + low, LANES), width)]
            values = jnp.concatenate(
                [own, own_next_ref[:, span], other_ref[:ROWS, span], other_next_ref[:, span]], axis=0
            )
            out_ref[:, here] = two_part_dot(table, values)
            out_ref[FLAGS:SENT, here] = flags


def meta_kernel(other_ref, meta_ref):
    meta_ref[...] = other_ref[ROWS:, :LANES]


def add_kernel(*refs):
    *got_refs, out_ref = refs
    for j in range(MEMBERS):
        lanes = slice(j * LANES, (j + 1) * LANES)
        six = [ref[FLAGS : FLAGS + 1, lanes] == 1.0 for ref in got_refs]
        eight = [ref[FLAGS + 1 : FLAGS + 2, lanes] == 1.0 for ref in got_refs]
        slot = lambda k, i: got_refs[k][BLOCK * i : BLOCK * (i + 1), lanes]
        terms = (
            lambda k: slot(k, 0),
            lambda k: slot(k, 1),
            lambda k: slot(k, 2),
            lambda k: jnp.where(six[k], slot(k, 3), 0.0),
            lambda k: slot(k, 4),
            lambda k: jnp.where(six[k], jnp.where(eight[k], 0.0, slot(k, 5)), slot(k, 3)),
            lambda k: jnp.where(eight[k], slot(k, 5), 0.0),
            lambda k: slot(k, 6),
            lambda k: got_refs[k][THERE:FLAGS, lanes],
        )
        for block, term in enumerate(terms):
            total = term(0)
            for k in range(1, MEMBERS):
                total = total + term(k)
            out_ref[j, BLOCK * block : BLOCK * block + total.shape[0], :] = total


def total_kernel(got_ref, out_ref):
    total = got_ref[0]
    for k in range(1, MEMBERS):
        total = total + got_ref[k]
    for k in range(MEMBERS):
        out_ref[k] = total


def pick_kernel(table_ref, *refs):
    for got_ref, out_ref in zip(refs[:MEMBERS], refs[MEMBERS:]):
        for j in range(MEMBERS):
            lanes = slice(j * LANES, (j + 1) * LANES)
            block = lambda i: table_ref[j, BLOCK * i : BLOCK * (i + 1), :]
            six = got_ref[FLAGS : FLAGS + 1, lanes] == 1.0
            eight = got_ref[FLAGS + 1 : FLAGS + 2, lanes] == 1.0
            out_ref[0:32, lanes] = block(0)
            out_ref[32:64, lanes] = block(1)
            out_ref[64:96, lanes] = block(2)
            out_ref[96:128, lanes] = jnp.where(six, block(3), block(5))
            out_ref[128:160, lanes] = block(4)
            out_ref[160:192, lanes] = jnp.where(eight, block(6), block(5))
            out_ref[192:224, lanes] = block(7)
            out_ref[THERE:FLAGS, lanes] = table_ref[j, 8 * BLOCK : TABLE, :]


def levels_in(level_ref, meta_ref):
    return level_ref[0] - LOW_LEVEL, number_in(meta_ref, 0).astype(jnp.int32) - LOW_LEVEL


def pieces(ref):
    width = ref.shape[1] // 2
    for h in range(2):
        yield h * width, ref[:, h * width : (h + 1) * width]


def other_back_kernel(level_ref, meta_ref, table_ref, *refs):
    *got_refs, out_ref = refs
    own, other = levels_in(level_ref, meta_ref)
    table = table_ref[other * 3 + own]
    for i, ref in enumerate(got_refs):
        for low, values in pieces(ref):
            out_ref[i, :, low : low + values.shape[1]] = two_part_dot(table, values)


def own_copies(turns, levels, table_ref, got_refs, out_ref, done_ref, sems):
    own, other = levels
    table = table_ref[own * 3 + other]
    first = core_here() * (out_ref.shape[1] // 2)
    i = 0
    for turn, ref in zip(turns, got_refs):
        for low, values in pieces(ref):
            width = values.shape[1]
            done_ref[i] = two_part_dot(table, values)
            start = pl.multiple_of(first + piece_here(turn) * ref.shape[1] + low, LANES)
            yield pltpu.make_async_copy(done_ref.at[i], out_ref.at[:, pl.ds(start, width)], sems.at[i])
            i += 1


def other_copies(turns, values_ref, out_ref, sems):
    first = (1 - core_here()) * (out_ref.shape[1] // 2)
    width = values_ref.shape[2]
    for i, turn in enumerate(turns):
        start = pl.multiple_of(first + (piece_here(turn) ^ 3) * width, LANES)
        yield pltpu.make_async_copy(values_ref.at[i], out_ref.at[:, pl.ds(start, width)], sems.at[i])


def run(*copies):
    started = []
    for group in copies:
        for copy in group:
            copy.start()
            started.append(copy)
    for copy in started:
        copy.wait()


def early_kernel(turns, level_ref, meta_ref, table_ref, *refs):
    *got_refs, out_ref, done_ref, sems = refs
    run(own_copies(turns, levels_in(level_ref, meta_ref), table_ref, got_refs, out_ref, done_ref, sems))


def late_kernel(turns, placed, level_ref, meta_ref, table_ref, *refs):
    *got_refs, values_ref, filled_ref, out_ref, done_ref, sems, other_sems = refs
    levels = levels_in(level_ref, meta_ref)
    run(
        other_copies(placed, values_ref, out_ref, other_sems),
        own_copies(turns, levels, table_ref, got_refs, out_ref, done_ref, sems),
    )


def place_kernel(turns, values_ref, filled_ref, out_ref, sems):
    run(other_copies(turns, values_ref, out_ref, sems))


def member(y, z, core):
    return (y % NY * NZ + z % NZ) * 2 + core


TILES = [
    [member(2 * a + i + core, 2 * b + j + core, core) for i in (0, 1) for j in (0, 1)]
    for core in (0, 1)
    for a in range(NY // 2)
    for b in range(NZ // 2)
]
ALONG_Y = [[[member(2 * a + i, z, core) for a in range(NY // 2)] for i in (0, 1) for z in range(NZ)] for core in (0, 1)]
ALONG_Z = [[[member(y, 2 * b + j, core) for b in range(NZ // 2)] for j in (0, 1) for y in range(NY)] for core in (0, 1)]
LINES = ALONG_Z[0] + ALONG_Y[1]
OTHER_LINES = ALONG_Y[0] + ALONG_Z[1]
VMEM = pl.BlockSpec(memory_space=pltpu.VMEM)
SMEM = pl.BlockSpec(memory_space=pltpu.SMEM)
HBM = pl.BlockSpec(memory_space=pltpu.HBM)
DMA = pltpu.SemaphoreType.DMA


def exchange(values, groups):
    return lax.all_to_all(values, "grp", 0, 0, axis_index_groups=groups, tiled=True)


def f32(*shape):
    return jax.ShapeDtypeStruct(shape, jnp.float32)


def call(kernel, ins, outs, shapes, scratch=(), limit=16, flops=0, moved=0, alias=None):
    return pl.pallas_call(
        kernel,
        in_specs=ins,
        out_specs=outs,
        out_shape=shapes,
        scratch_shapes=scratch,
        compiler_params=pltpu.CompilerParams(vmem_limit_bytes=limit << 20),
        cost_estimate=pl.CostEstimate(flops=flops, bytes_accessed=moved, transcendentals=0),
        input_output_aliases=alias or {},
    )


def shards(grids, first_level, coeffs, slot_map):
    rows = grids[0]
    width = rows.shape[1]
    half = width // 2
    chunk = half // MEMBERS
    slabs = lax.axis_size("slab")
    members = lax.axis_size("grp")
    swap = [(i, i ^ 1) for i in range(members)]
    forth, back = (jnp.asarray(table, jnp.bfloat16) for table in row_tables())

    def to_previous(values, turn):
        pairs = [
            (g * slabs + s, (g ^ turn) * slabs + (s - 1) % slabs)
            for g in range(members)
            for s in range(slabs)
        ]
        return lax.ppermute(values, ("grp", "slab"), pairs)

    def through_tile(pieces):
        turned = lambda turn: [(tile[i], tile[i ^ turn]) for tile in TILES for i in range(MEMBERS)]
        far = {}
        for turn in (3, 2, 1):
            far[turn] = lax.ppermute(pieces[turn], "grp", turned(turn))
        return [pieces[0], far[1], far[2], far[3]]

    line = call(lead_kernel, [], VMEM, jax.ShapeDtypeStruct((8, LANES), jnp.int32), flops=2*10**9)()
    numbers = call(numbers_kernel, [SMEM, SMEM, VMEM], VMEM, f32(8, LANES))(first_level, coeffs, line)
    entry, own_plane, other_plane = call(
        entry_kernel, [VMEM] * 2, [VMEM] * 3,
        [f32(ROWS + 8, half), f32(PLANE, half), f32(PLANE, half)],
    )(numbers, rows)
    other_next = to_previous(other_plane, 1)
    own_next = to_previous(own_plane, 0)
    other = lax.ppermute(entry, "grp", swap)

    def surplus(*turns):
        return call(
            functools.partial(forth_kernel, turns), [SMEM, SMEM] + [VMEM] * 5, [VMEM] * len(turns),
            [f32(SENT, chunk)] * len(turns), flops=10**9,
        )(first_level, coeffs, forth, rows, own_next, other, other_next)

    sent = surplus(1, 2, 3)
    (stays,) = surplus(0)
    meta = call(meta_kernel, [VMEM], VMEM, f32(8, LANES))(other)
    got = through_tile([stays, *sent])

    parts = call(add_kernel, [VMEM] * MEMBERS, VMEM, f32(MEMBERS, TABLE, LANES), flops=10**8)(*got)
    for groups in (LINES, OTHER_LINES):
        parts = exchange(parts, groups)
        parts = call(total_kernel, [VMEM], VMEM, f32(MEMBERS, TABLE, LANES), flops=10**8)(parts)
    table = exchange(parts, LINES)
    picked = call(
        pick_kernel, [VMEM] * (MEMBERS + 1), [VMEM] * MEMBERS, [f32(FLAGS, chunk)] * MEMBERS, flops=10**8
    )(table, *got)
    final = through_tile(picked)

    def other_rows(turns):
        return call(
            other_back_kernel, [SMEM] + [VMEM] * (2 + len(turns)), VMEM,
            f32(len(turns), ROWS, chunk), flops=10**9,
        )(first_level, meta, back, *[final[turn] for turn in turns])

    parts = (pltpu.VMEM((4, ROWS, chunk // 2), jnp.float32), DMA((4,)))

    def own_early_rows(turns):
        return call(
            functools.partial(early_kernel, turns), [SMEM] + [VMEM] * 4, HBM, f32(ROWS, width),
            parts, flops=10**9,
        )(first_level, meta, back, *[final[turn] for turn in turns])

    def own_late_rows(turns, placed, values, filled):
        return call(
            functools.partial(late_kernel, turns, placed), [SMEM] + [VMEM] * 5 + [HBM], HBM,
            f32(ROWS, width), (*parts, DMA((2,))), flops=10**9, alias={6: 0},
        )(first_level, meta, back, *[final[turn] for turn in turns], values, filled)

    def place(turns, values, filled):
        return call(
            functools.partial(place_kernel, turns), [VMEM, HBM], HBM, f32(ROWS, width),
            (DMA((2,)),), alias={1: 0}, flops=10**8,
        )(values, filled)

    early, late = (0, 3), (2, 1)
    other_early = other_rows(early)
    swapped_early = lax.ppermute(other_early, "grp", swap)
    out = own_early_rows(early)
    other_late = other_rows(late)
    swapped_late = lax.ppermute(other_late, "grp", swap)
    out = own_late_rows(late, early, swapped_early, out)
    out = place(late, swapped_late, out)
    return out[None]


def solution(mesh):
    in_specs = (P("grp", "slab", None), P("grp"), P("grp"), P("grp", "slab"))
    out_specs = P("grp", "slab", None)
    return jax.shard_map(shards, mesh=mesh, in_specs=in_specs, out_specs=out_specs, check_vma=False)
```

```python
import functools

import jax
import jax.numpy as jnp
import numpy as np
from jax import lax
from jax.experimental import pallas as pl
from jax.experimental.pallas import tpu as pltpu
from jax.sharding import PartitionSpec as P

LEVEL_SUM = 9
LOW_LEVEL = 6
NY = 8
NZ = 8
MEMBERS = 4
ROWS = 128
PLANE = 8
BLOCK = 32
SLOTS = 7
THERE = SLOTS * BLOCK
FLAGS = THERE + PLANE
SENT = FLAGS + 8
ENTRY = 2 * (ROWS + PLANE)
TABLE = 8 * BLOCK + PLANE
LANES = 128


def slots_of(levels):
    six, seven, eight = (level in levels for level in (6, 7, 8))
    third = 3 if six else (5 if seven else None)
    fifth = 6 if eight else (5 if six and seven else None)
    return (0, 1, 2, third, 4, fifth, 7)


def place_of(x, y):
    if x % 4 == 0 and y % 4 == 0:
        return (x // 4) * 2 + y // 4
    if x % 4 == 0 and y % 2 == 0:
        return 32 + (x // 4) * 2 + y // 4
    if x % 4 == 2 and y % 4 == 0:
        return 64 + (x // 4) * 2 + y // 4
    if x % 4 == 0:
        return 96 + (x // 4) * 4 + y // 2
    if x % 4 == 2:
        return 160 + (x // 4) * 2 + y // 4
    return 192 + (x // 2) * 2 + y // 4


def hier_line(n):
    h = np.zeros((n, n), np.float32)
    for j in range(n):
        h[j, j] += 1.0
        if j:
            s = j & -j
            h[j, j - s] -= 0.5
            h[j, (j + s) % n] -= 0.5
    return h


def dehier_line(n):
    e = np.zeros((n, n), np.float32)
    e[:, 0] = 1.0
    for k in range(1, n):
        for j in range(n):
            d = min(abs(j - k), n - abs(j - k))
            e[j, k] = max(0.0, 1.0 - d / (k & -k))
    return e


def one_grid(level, slots):
    n = 1 << (LEVEL_SUM - level)
    span = ROWS // n
    hy, ey = hier_line(n), dehier_line(n)
    forth = np.zeros((SENT, ROWS + PLANE), np.float32)
    back = np.zeros((ROWS, FLAGS), np.float32)
    for i in range(span):
        for y in range(n):
            t = place_of(i * 64 // span, y * 8 // n)
            m = BLOCK * slots.index(t // BLOCK) + t % BLOCK
            s = i & -i
            steps = [(i, 1.0)] + ([(i - s, -0.5), (i + s, -0.5)] if i else [])
            for j, w in steps:
                forth[m, j * n : j * n + n] += w * hy[y]
            for j in range(span):
                w = max(0.0, 1.0 - abs(j - i) / s) if i else 1.0 - j / span
                back[j * n : j * n + n, m] += w * ey[:, y]
    for y in range(n):
        t = THERE + y * 8 // n
        forth[t, ROWS : ROWS + n] += hy[y]
        for j in range(span):
            back[j * n : j * n + n, t] += j / span * ey[:, y]
    return forth, back


@functools.cache
def row_tables():
    forth, back = [], []
    for own in (6, 7, 8):
        for other in (6, 7, 8):
            slots = slots_of((own, other))
            mine, theirs = one_grid(own, slots), one_grid(other, slots)
            parts = [grid[0][:, span] for span in (slice(ROWS), slice(ROWS, None)) for grid in (mine, theirs)]
            forth.append(np.concatenate(parts, axis=1))
            back.append(mine[1])
    return np.stack(forth), np.stack(back)


def two_part_dot(table, values):
    high = values.astype(jnp.bfloat16)
    low = (values - high.astype(jnp.float32)).astype(jnp.bfloat16)
    dot = functools.partial(jnp.dot, preferred_element_type=jnp.float32)
    return dot(table, high) + dot(table, low)


def number_in(ref, row):
    return jnp.max(ref[row : row + 1, :LANES])


def core_here():
    return lax.axis_index("grp") % 2


def piece_here(turn):
    me = lax.axis_index("grp")
    core, z, y = me % 2, me // 2 % NZ, me // (2 * NZ)
    return ((y + core) % 2 * 2 + (z + core) % 2) ^ turn


def lead_kernel(out_ref):
    out_ref[...] = lax.broadcasted_iota(jnp.int32, out_ref.shape, 0)


def numbers_kernel(level_ref, coeff_ref, line_ref, out_ref):
    out_ref[...] = jnp.where(line_ref[...] == 0, level_ref[0], coeff_ref[0]).astype(jnp.float32)


def halves(width):
    half, core = width // 2, core_here()
    return [pl.multiple_of(which * half, LANES) for which in (core, 1 - core)]


def entry_kernel(numbers_ref, rows_ref, out_ref, plane_ref):
    half = out_ref.shape[1]
    _, theirs = halves(rows_ref.shape[1])
    plane_ref[...] = rows_ref[:PLANE, :]
    out_ref[:ROWS, :] = rows_ref[:, pl.ds(theirs, half)]
    out_ref[ROWS:, :] = jnp.concatenate([numbers_ref[...]] * (half // LANES), axis=1)


def cut_kernel(plane_ref, out_ref):
    _, theirs = halves(plane_ref.shape[1])
    out_ref[...] = plane_ref[:, pl.ds(theirs, out_ref.shape[1])]


def pair_of(level_ref, other_ref):
    return level_ref[0], number_in(other_ref, ROWS).astype(jnp.int32)


def scaled(table, coeff_ref, other_ref, part):
    lane = lax.broadcasted_iota(jnp.int32, (1, part.stop - part.start), 1)
    own = lane < (part.stop - part.start) // 2
    scale = jnp.where(own, coeff_ref[0].astype(jnp.float32), number_in(other_ref, ROWS + 1))
    return (table[:, part].astype(jnp.float32) * scale).astype(jnp.bfloat16)


MAIN, NEXT = slice(0, 2 * ROWS), slice(2 * ROWS, ENTRY)


def windows(turn, chunk):
    width = chunk // 2
    for h in range(2):
        low = pl.multiple_of(piece_here(turn) * chunk + h * width, LANES)
        yield slice(h * width, (h + 1) * width), low, width


def main_kernel(turns, level_ref, coeff_ref, table_ref, rows_ref, other_ref, *out_refs):
    own_level, other_level = pair_of(level_ref, other_ref)
    table = table_ref[(own_level - LOW_LEVEL) * 3 + other_level - LOW_LEVEL]
    table = scaled(table, coeff_ref, other_ref, MAIN)
    six = jnp.logical_or(own_level == 6, other_level == 6).astype(jnp.float32)
    eight = jnp.logical_or(own_level == 8, other_level == 8).astype(jnp.float32)
    chunk = out_refs[0].shape[1]
    line = lax.broadcasted_iota(jnp.int32, (SENT - FLAGS, chunk // 2), 0)
    flags = jnp.where(line == 0, six, eight)
    first, _ = halves(rows_ref.shape[1])
    for turn, out_ref in zip(turns, out_refs):
        for here, low, width in windows(turn, chunk):
            own = rows_ref[:, pl.ds(pl.multiple_of(first + low, LANES), width)]
            values = jnp.concatenate([own, other_ref[:ROWS, pl.ds(low, width)]], axis=0)
            out_ref[:, here] = two_part_dot(table, values)
            out_ref[FLAGS:SENT, here] = flags


def next_kernel(turns, level_ref, coeff_ref, table_ref, plane_ref, other_ref, other_next_ref, *refs):
    got_refs, out_refs = refs[: len(turns)], refs[len(turns) :]
    own_level, other_level = pair_of(level_ref, other_ref)
    table = table_ref[(own_level - LOW_LEVEL) * 3 + other_level - LOW_LEVEL]
    table = scaled(table, coeff_ref, other_ref, NEXT)
    chunk = out_refs[0].shape[1]
    first, _ = halves(plane_ref.shape[1])
    for turn, got_ref, out_ref in zip(turns, got_refs, out_refs):
        for here, low, width in windows(turn, chunk):
            own = plane_ref[:, pl.ds(pl.multiple_of(first + low, LANES), width)]
            values = jnp.concatenate([own, other_next_ref[:, pl.ds(low, width)]], axis=0)
            out_ref[:, here] = got_ref[:, here] + two_part_dot(table, values)


def meta_kernel(other_ref, meta_ref):
    meta_ref[...] = other_ref[ROWS:, :LANES]


def add_kernel(*refs):
    *got_refs, out_ref = refs
    for j in range(MEMBERS):
        lanes = slice(j * LANES, (j + 1) * LANES)
        six = [ref[FLAGS : FLAGS + 1, lanes] == 1.0 for ref in got_refs]
        eight = [ref[FLAGS + 1 : FLAGS + 2, lanes] == 1.0 for ref in got_refs]
        slot = lambda k, i: got_refs[k][BLOCK * i : BLOCK * (i + 1), lanes]
        terms = (
            lambda k: slot(k, 0),
            lambda k: slot(k, 1),
            lambda k: slot(k, 2),
            lambda k: jnp.where(six[k], slot(k, 3), 0.0),
            lambda k: slot(k, 4),
            lambda k: jnp.where(six[k], jnp.where(eight[k], 0.0, slot(k, 5)), slot(k, 3)),
            lambda k: jnp.where(eight[k], slot(k, 5), 0.0),
            lambda k: slot(k, 6),
            lambda k: got_refs[k][THERE:FLAGS, lanes],
        )
        for block, term in enumerate(terms):
            total = term(0)
            for k in range(1, MEMBERS):
                total = total + term(k)
            out_ref[j, BLOCK * block : BLOCK * block + total.shape[0], :] = total


def total_kernel(got_ref, out_ref):
    total = got_ref[0]
    for k in range(1, MEMBERS):
        total = total + got_ref[k]
    for k in range(MEMBERS):
        out_ref[k] = total


def pick_kernel(table_ref, *refs):
    for got_ref, out_ref in zip(refs[:MEMBERS], refs[MEMBERS:]):
        for j in range(MEMBERS):
            lanes = slice(j * LANES, (j + 1) * LANES)
            block = lambda i: table_ref[j, BLOCK * i : BLOCK * (i + 1), :]
            six = got_ref[FLAGS : FLAGS + 1, lanes] == 1.0
            eight = got_ref[FLAGS + 1 : FLAGS + 2, lanes] == 1.0
            out_ref[0:32, lanes] = block(0)
            out_ref[32:64, lanes] = block(1)
            out_ref[64:96, lanes] = block(2)
            out_ref[96:128, lanes] = jnp.where(six, block(3), block(5))
            out_ref[128:160, lanes] = block(4)
            out_ref[160:192, lanes] = jnp.where(eight, block(6), block(5))
            out_ref[192:224, lanes] = block(7)
            out_ref[THERE:FLAGS, lanes] = table_ref[j, 8 * BLOCK : TABLE, :]


def levels_in(level_ref, meta_ref):
    return level_ref[0] - LOW_LEVEL, number_in(meta_ref, 0).astype(jnp.int32) - LOW_LEVEL


def pieces(ref):
    width = ref.shape[1] // 2
    for h in range(2):
        yield h * width, ref[:, h * width : (h + 1) * width]


def other_back_kernel(level_ref, meta_ref, table_ref, *refs):
    *got_refs, out_ref = refs
    own, other = levels_in(level_ref, meta_ref)
    table = table_ref[other * 3 + own]
    for i, ref in enumerate(got_refs):
        for low, values in pieces(ref):
            out_ref[i, :, low : low + values.shape[1]] = two_part_dot(table, values)


def own_copies(turns, levels, table_ref, got_refs, out_ref, done_ref, sems):
    own, other = levels
    table = table_ref[own * 3 + other]
    first = core_here() * (out_ref.shape[1] // 2)
    i = 0
    for turn, ref in zip(turns, got_refs):
        for low, values in pieces(ref):
            width = values.shape[1]
            done_ref[i] = two_part_dot(table, values)
            start = pl.multiple_of(first + piece_here(turn) * ref.shape[1] + low, LANES)
            yield pltpu.make_async_copy(done_ref.at[i], out_ref.at[:, pl.ds(start, width)], sems.at[i])
            i += 1


def other_copies(turns, values_ref, out_ref, sems):
    first = (1 - core_here()) * (out_ref.shape[1] // 2)
    width = values_ref.shape[2]
    for i, turn in enumerate(turns):
        start = pl.multiple_of(first + (piece_here(turn) ^ 3) * width, LANES)
        yield pltpu.make_async_copy(values_ref.at[i], out_ref.at[:, pl.ds(start, width)], sems.at[i])


def run(*copies):
    started = []
    for group in copies:
        for copy in group:
            copy.start()
            started.append(copy)
    for copy in started:
        copy.wait()


def early_kernel(turns, level_ref, meta_ref, table_ref, *refs):
    *got_refs, out_ref, done_ref, sems = refs
    run(own_copies(turns, levels_in(level_ref, meta_ref), table_ref, got_refs, out_ref, done_ref, sems))


def late_kernel(turns, placed, level_ref, meta_ref, table_ref, *refs):
    *got_refs, values_ref, filled_ref, out_ref, done_ref, sems, other_sems = refs
    levels = levels_in(level_ref, meta_ref)
    run(
        other_copies(placed, values_ref, out_ref, other_sems),
        own_copies(turns, levels, table_ref, got_refs, out_ref, done_ref, sems),
    )


def place_kernel(turns, values_ref, filled_ref, out_ref, sems):
    run(other_copies(turns, values_ref, out_ref, sems))


def member(y, z, core):
    return (y % NY * NZ + z % NZ) * 2 + core


TILES = [
    [member(2 * a + i + core, 2 * b + j + core, core) for i in (0, 1) for j in (0, 1)]
    for core in (0, 1)
    for a in range(NY // 2)
    for b in range(NZ // 2)
]
ALONG_Y = [[[member(2 * a + i, z, core) for a in range(NY // 2)] for i in (0, 1) for z in range(NZ)] for core in (0, 1)]
ALONG_Z = [[[member(y, 2 * b + j, core) for b in range(NZ // 2)] for j in (0, 1) for y in range(NY)] for core in (0, 1)]
LINES = ALONG_Z[0] + ALONG_Y[1]
OTHER_LINES = ALONG_Y[0] + ALONG_Z[1]
VMEM = pl.BlockSpec(memory_space=pltpu.VMEM)
SMEM = pl.BlockSpec(memory_space=pltpu.SMEM)
HBM = pl.BlockSpec(memory_space=pltpu.HBM)
DMA = pltpu.SemaphoreType.DMA


def exchange(values, groups):
    return lax.all_to_all(values, "grp", 0, 0, axis_index_groups=groups, tiled=True)


def f32(*shape):
    return jax.ShapeDtypeStruct(shape, jnp.float32)


def call(kernel, ins, outs, shapes, scratch=(), limit=16, flops=0, moved=0, alias=None):
    return pl.pallas_call(
        kernel,
        in_specs=ins,
        out_specs=outs,
        out_shape=shapes,
        scratch_shapes=scratch,
        compiler_params=pltpu.CompilerParams(vmem_limit_bytes=limit << 20),
        cost_estimate=pl.CostEstimate(flops=flops, bytes_accessed=moved, transcendentals=0),
        input_output_aliases=alias or {},
    )


def shards(grids, first_level, coeffs, slot_map):
    rows = grids[0]
    width = rows.shape[1]
    half = width // 2
    chunk = half // MEMBERS
    slabs = lax.axis_size("slab")
    members = lax.axis_size("grp")
    swap = [(i, i ^ 1) for i in range(members)]
    forth, back = (jnp.asarray(table, jnp.bfloat16) for table in row_tables())

    to_previous = [(i, (i - 1) % slabs) for i in range(slabs)]

    def through_tile(pieces):
        turned = lambda turn: [(tile[i], tile[i ^ turn]) for tile in TILES for i in range(MEMBERS)]
        far = {}
        for turn in (3, 2, 1):
            far[turn] = lax.ppermute(pieces[turn], "grp", turned(turn))
        return [pieces[0], far[1], far[2], far[3]]

    line = call(lead_kernel, [], VMEM, jax.ShapeDtypeStruct((8, LANES), jnp.int32), flops=2*10**9)()
    numbers = call(numbers_kernel, [SMEM, SMEM, VMEM], VMEM, f32(8, LANES))(first_level, coeffs, line)
    entry, plane = call(entry_kernel, [VMEM] * 2, [VMEM] * 2, [f32(ROWS + 8, half), f32(PLANE, width)])(numbers, rows)

    def main_part(*turns):
        return call(
            functools.partial(main_kernel, turns), [SMEM, SMEM] + [VMEM] * 3, [VMEM] * len(turns),
            [f32(SENT, chunk)] * len(turns), flops=10**9,
        )(first_level, coeffs, forth, rows, other)

    def with_next(got, *turns):
        count = len(turns)
        return call(
            functools.partial(next_kernel, turns), [SMEM, SMEM] + [VMEM] * (4 + count), [VMEM] * count,
            [f32(SENT, chunk)] * count, flops=10**8, alias={6 + i: i for i in range(count)},
        )(first_level, coeffs, forth, next_plane, other, other_next, *got)

    next_plane = lax.ppermute(plane, "slab", to_previous)
    other = lax.ppermute(entry, "grp", swap)
    cut = call(cut_kernel, [VMEM], VMEM, f32(PLANE, half))(next_plane)
    other_next = lax.ppermute(cut, "grp", swap)
    sent = main_part(1, 2, 3)
    sent = with_next(sent, 1, 2, 3)
    (stays,) = with_next(main_part(0), 0)
    meta = call(meta_kernel, [VMEM], VMEM, f32(8, LANES))(other)
    got = through_tile([stays, *sent])

    parts = call(add_kernel, [VMEM] * MEMBERS, VMEM, f32(MEMBERS, TABLE, LANES), flops=10**8)(*got)
    for groups in (LINES, OTHER_LINES):
        parts = exchange(parts, groups)
        parts = call(total_kernel, [VMEM], VMEM, f32(MEMBERS, TABLE, LANES), flops=10**8)(parts)
    table = exchange(parts, LINES)
    picked = call(
        pick_kernel, [VMEM] * (MEMBERS + 1), [VMEM] * MEMBERS, [f32(FLAGS, chunk)] * MEMBERS, flops=10**8
    )(table, *got)
    final = through_tile(picked)

    def other_rows(turns):
        return call(
            other_back_kernel, [SMEM] + [VMEM] * (2 + len(turns)), VMEM,
            f32(len(turns), ROWS, chunk), flops=10**9,
        )(first_level, meta, back, *[final[turn] for turn in turns])

    parts = (pltpu.VMEM((4, ROWS, chunk // 2), jnp.float32), DMA((4,)))

    def own_early_rows(turns):
        return call(
            functools.partial(early_kernel, turns), [SMEM] + [VMEM] * 4, HBM, f32(ROWS, width),
            parts, flops=10**9,
        )(first_level, meta, back, *[final[turn] for turn in turns])

    def own_late_rows(turns, placed, values, filled):
        return call(
            functools.partial(late_kernel, turns, placed), [SMEM] + [VMEM] * 5 + [HBM], HBM,
            f32(ROWS, width), (*parts, DMA((2,))), flops=10**9, alias={6: 0},
        )(first_level, meta, back, *[final[turn] for turn in turns], values, filled)

    def place(turns, values, filled):
        return call(
            functools.partial(place_kernel, turns), [VMEM, HBM], HBM, f32(ROWS, width),
            (DMA((2,)),), alias={1: 0}, flops=10**8,
        )(values, filled)

    early, late = (0, 3), (2, 1)
    other_early = other_rows(early)
    swapped_early = lax.ppermute(other_early, "grp", swap)
    out = own_early_rows(early)
    other_late = other_rows(late)
    swapped_late = lax.ppermute(other_late, "grp", swap)
    out = own_late_rows(late, early, swapped_early, out)
    out = place(late, swapped_late, out)
    return out[None]


def solution(mesh):
    in_specs = (P("grp", "slab", None), P("grp"), P("grp"), P("grp", "slab"))
    out_specs = P("grp", "slab", None)
    return jax.shard_map(shards, mesh=mesh, in_specs=in_specs, out_specs=out_specs, check_vma=False)
```

```python
import functools

import jax
import jax.numpy as jnp
import numpy as np
from jax import lax
from jax.experimental import pallas as pl
from jax.experimental.pallas import tpu as pltpu
from jax.sharding import PartitionSpec as P

LEVEL_SUM = 9
LOW_LEVEL = 6
NY = 8
NZ = 8
MEMBERS = 4
ROWS = 128
PLANE = 8
BLOCK = 32
SLOTS = 7
THERE = SLOTS * BLOCK
FLAGS = THERE + PLANE
SENT = FLAGS + 8
ENTRY = 2 * (ROWS + PLANE)
TABLE = 8 * BLOCK + PLANE
LANES = 128


def slots_of(levels):
    six, seven, eight = (level in levels for level in (6, 7, 8))
    third = 3 if six else (5 if seven else None)
    fifth = 6 if eight else (5 if six and seven else None)
    return (0, 1, 2, third, 4, fifth, 7)


def place_of(x, y):
    if x % 4 == 0 and y % 4 == 0:
        return (x // 4) * 2 + y // 4
    if x % 4 == 0 and y % 2 == 0:
        return 32 + (x // 4) * 2 + y // 4
    if x % 4 == 2 and y % 4 == 0:
        return 64 + (x // 4) * 2 + y // 4
    if x % 4 == 0:
        return 96 + (x // 4) * 4 + y // 2
    if x % 4 == 2:
        return 160 + (x // 4) * 2 + y // 4
    return 192 + (x // 2) * 2 + y // 4


def hier_line(n):
    h = np.zeros((n, n), np.float32)
    for j in range(n):
        h[j, j] += 1.0
        if j:
            s = j & -j
            h[j, j - s] -= 0.5
            h[j, (j + s) % n] -= 0.5
    return h


def dehier_line(n):
    e = np.zeros((n, n), np.float32)
    e[:, 0] = 1.0
    for k in range(1, n):
        for j in range(n):
            d = min(abs(j - k), n - abs(j - k))
            e[j, k] = max(0.0, 1.0 - d / (k & -k))
    return e


def one_grid(level, slots):
    n = 1 << (LEVEL_SUM - level)
    span = ROWS // n
    hy, ey = hier_line(n), dehier_line(n)
    forth = np.zeros((SENT, ROWS + PLANE), np.float32)
    back = np.zeros((ROWS, FLAGS), np.float32)
    for i in range(span):
        for y in range(n):
            t = place_of(i * 64 // span, y * 8 // n)
            m = BLOCK * slots.index(t // BLOCK) + t % BLOCK
            s = i & -i
            steps = [(i, 1.0)] + ([(i - s, -0.5), (i + s, -0.5)] if i else [])
            for j, w in steps:
                forth[m, j * n : j * n + n] += w * hy[y]
            for j in range(span):
                w = max(0.0, 1.0 - abs(j - i) / s) if i else 1.0 - j / span
                back[j * n : j * n + n, m] += w * ey[:, y]
    for y in range(n):
        t = THERE + y * 8 // n
        forth[t, ROWS : ROWS + n] += hy[y]
        for j in range(span):
            back[j * n : j * n + n, t] += j / span * ey[:, y]
    return forth, back


@functools.cache
def row_tables():
    forth, back = [], []
    for own in (6, 7, 8):
        for other in (6, 7, 8):
            slots = slots_of((own, other))
            mine, theirs = one_grid(own, slots), one_grid(other, slots)
            parts = [grid[0][:, span] for span in (slice(ROWS), slice(ROWS, None)) for grid in (mine, theirs)]
            forth.append(np.concatenate(parts, axis=1))
            back.append(mine[1])
    return np.stack(forth), np.stack(back)


def two_part_dot(table, values):
    high = values.astype(jnp.bfloat16)
    low = (values - high.astype(jnp.float32)).astype(jnp.bfloat16)
    dot = functools.partial(jnp.dot, preferred_element_type=jnp.float32)
    return dot(table, high) + dot(table, low)


def number_in(ref, row):
    return jnp.max(ref[row : row + 1, :LANES])


def core_here():
    return lax.axis_index("grp") % 2


def piece_here(turn):
    me = lax.axis_index("grp")
    core, z, y = me % 2, me // 2 % NZ, me // (2 * NZ)
    return ((y + core) % 2 * 2 + (z + core) % 2) ^ turn


def lead_kernel(out_ref):
    out_ref[...] = lax.broadcasted_iota(jnp.int32, out_ref.shape, 0)


def numbers_kernel(level_ref, coeff_ref, line_ref, out_ref):
    out_ref[...] = jnp.where(line_ref[...] == 0, level_ref[0], coeff_ref[0]).astype(jnp.float32)


def halves(width):
    half, core = width // 2, core_here()
    return [pl.multiple_of(which * half, LANES) for which in (core, 1 - core)]


def entry_kernel(numbers_ref, rows_ref, out_ref, plane_ref):
    half = out_ref.shape[1]
    _, theirs = halves(rows_ref.shape[1])
    plane_ref[...] = rows_ref[:PLANE, :]
    out_ref[:ROWS, :] = rows_ref[:, pl.ds(theirs, half)]
    out_ref[ROWS:, :] = jnp.concatenate([numbers_ref[...]] * (half // LANES), axis=1)


def cut_kernel(plane_ref, out_ref):
    _, theirs = halves(plane_ref.shape[1])
    out_ref[...] = plane_ref[:, pl.ds(theirs, out_ref.shape[1])]


def pair_of(level_ref, other_ref):
    return level_ref[0], number_in(other_ref, ROWS).astype(jnp.int32)


def scaled(table, coeff_ref, other_ref, part):
    lane = lax.broadcasted_iota(jnp.int32, (1, part.stop - part.start), 1)
    own = lane < (part.stop - part.start) // 2
    scale = jnp.where(own, coeff_ref[0].astype(jnp.float32), number_in(other_ref, ROWS + 1))
    return (table[:, part].astype(jnp.float32) * scale).astype(jnp.bfloat16)


MAIN, NEXT = slice(0, 2 * ROWS), slice(2 * ROWS, ENTRY)


def windows(turn, chunk):
    width = chunk // 2
    for h in range(2):
        low = pl.multiple_of(piece_here(turn) * chunk + h * width, LANES)
        yield slice(h * width, (h + 1) * width), low, width


def main_kernel(turns, level_ref, coeff_ref, table_ref, rows_ref, other_ref, *out_refs):
    own_level, other_level = pair_of(level_ref, other_ref)
    table = table_ref[(own_level - LOW_LEVEL) * 3 + other_level - LOW_LEVEL]
    table = scaled(table, coeff_ref, other_ref, MAIN)
    six = jnp.logical_or(own_level == 6, other_level == 6).astype(jnp.float32)
    eight = jnp.logical_or(own_level == 8, other_level == 8).astype(jnp.float32)
    chunk = out_refs[0].shape[1]
    line = lax.broadcasted_iota(jnp.int32, (SENT - FLAGS, chunk // 2), 0)
    flags = jnp.where(line == 0, six, eight)
    first, _ = halves(rows_ref.shape[1])
    for turn, out_ref in zip(turns, out_refs):
        for here, low, width in windows(turn, chunk):
            own = rows_ref[:, pl.ds(pl.multiple_of(first + low, LANES), width)]
            values = jnp.concatenate([own, other_ref[:ROWS, pl.ds(low, width)]], axis=0)
            out_ref[:, here] = two_part_dot(table, values)
            out_ref[FLAGS:SENT, here] = flags


def next_kernel(turns, level_ref, coeff_ref, table_ref, plane_ref, other_ref, other_next_ref, *refs):
    got_refs, out_refs = refs[: len(turns)], refs[len(turns) :]
    own_level, other_level = pair_of(level_ref, other_ref)
    table = table_ref[(own_level - LOW_LEVEL) * 3 + other_level - LOW_LEVEL]
    table = scaled(table, coeff_ref, other_ref, NEXT)
    chunk = out_refs[0].shape[1]
    first, _ = halves(plane_ref.shape[1])
    for turn, got_ref, out_ref in zip(turns, got_refs, out_refs):
        for here, low, width in windows(turn, chunk):
            own = plane_ref[:, pl.ds(pl.multiple_of(first + low, LANES), width)]
            values = jnp.concatenate([own, other_next_ref[:, pl.ds(low, width)]], axis=0)
            out_ref[:, here] = got_ref[:, here] + two_part_dot(table, values)


def meta_kernel(other_ref, meta_ref):
    meta_ref[...] = other_ref[ROWS:, :LANES]


def add_kernel(*refs):
    *got_refs, out_ref = refs
    for j in range(MEMBERS):
        lanes = slice(j * LANES, (j + 1) * LANES)
        six = [ref[FLAGS : FLAGS + 1, lanes] == 1.0 for ref in got_refs]
        eight = [ref[FLAGS + 1 : FLAGS + 2, lanes] == 1.0 for ref in got_refs]
        slot = lambda k, i: got_refs[k][BLOCK * i : BLOCK * (i + 1), lanes]
        terms = (
            lambda k: slot(k, 0),
            lambda k: slot(k, 1),
            lambda k: slot(k, 2),
            lambda k: jnp.where(six[k], slot(k, 3), 0.0),
            lambda k: slot(k, 4),
            lambda k: jnp.where(six[k], jnp.where(eight[k], 0.0, slot(k, 5)), slot(k, 3)),
            lambda k: jnp.where(eight[k], slot(k, 5), 0.0),
            lambda k: slot(k, 6),
            lambda k: got_refs[k][THERE:FLAGS, lanes],
        )
        for block, term in enumerate(terms):
            total = term(0)
            for k in range(1, MEMBERS):
                total = total + term(k)
            out_ref[j, BLOCK * block : BLOCK * block + total.shape[0], :] = total


def total_kernel(got_ref, out_ref):
    total = got_ref[0]
    for k in range(1, MEMBERS):
        total = total + got_ref[k]
    for k in range(MEMBERS):
        out_ref[k] = total


def pick_kernel(table_ref, *refs):
    for got_ref, out_ref in zip(refs[:MEMBERS], refs[MEMBERS:]):
        for j in range(MEMBERS):
            lanes = slice(j * LANES, (j + 1) * LANES)
            block = lambda i: table_ref[j, BLOCK * i : BLOCK * (i + 1), :]
            six = got_ref[FLAGS : FLAGS + 1, lanes] == 1.0
            eight = got_ref[FLAGS + 1 : FLAGS + 2, lanes] == 1.0
            out_ref[0:32, lanes] = block(0)
            out_ref[32:64, lanes] = block(1)
            out_ref[64:96, lanes] = block(2)
            out_ref[96:128, lanes] = jnp.where(six, block(3), block(5))
            out_ref[128:160, lanes] = block(4)
            out_ref[160:192, lanes] = jnp.where(eight, block(6), block(5))
            out_ref[192:224, lanes] = block(7)
            out_ref[THERE:FLAGS, lanes] = table_ref[j, 8 * BLOCK : TABLE, :]


def levels_in(level_ref, meta_ref):
    return level_ref[0] - LOW_LEVEL, number_in(meta_ref, 0).astype(jnp.int32) - LOW_LEVEL


def pieces(ref):
    width = ref.shape[1] // 2
    for h in range(2):
        yield h * width, ref[:, h * width : (h + 1) * width]


def other_back_kernel(level_ref, meta_ref, table_ref, *refs):
    *got_refs, out_ref = refs
    own, other = levels_in(level_ref, meta_ref)
    table = table_ref[other * 3 + own]
    for i, ref in enumerate(got_refs):
        for low, values in pieces(ref):
            out_ref[i, :, low : low + values.shape[1]] = two_part_dot(table, values)


def own_copies(turns, levels, table_ref, got_refs, out_ref, done_ref, sems):
    own, other = levels
    table = table_ref[own * 3 + other]
    first = core_here() * (out_ref.shape[1] // 2)
    i = 0
    for turn, ref in zip(turns, got_refs):
        for low, values in pieces(ref):
            width = values.shape[1]
            done_ref[i] = two_part_dot(table, values)
            start = pl.multiple_of(first + piece_here(turn) * ref.shape[1] + low, LANES)
            yield pltpu.make_async_copy(done_ref.at[i], out_ref.at[:, pl.ds(start, width)], sems.at[i])
            i += 1


def piece_copies(turns, core, flip, values_ref, out_ref, sems):
    first = core * (out_ref.shape[1] // 2)
    width = values_ref.shape[2]
    for i, turn in enumerate(turns):
        start = pl.multiple_of(first + (piece_here(turn) ^ flip) * width, LANES)
        yield pltpu.make_async_copy(values_ref.at[i], out_ref.at[:, pl.ds(start, width)], sems.at[i])


def run(*copies):
    started = []
    for group in copies:
        for copy in group:
            copy.start()
            started.append(copy)
    for copy in started:
        copy.wait()


def early_kernel(turns, level_ref, meta_ref, table_ref, *refs):
    *got_refs, out_ref, done_ref, sems = refs
    run(own_copies(turns, levels_in(level_ref, meta_ref), table_ref, got_refs, out_ref, done_ref, sems))


def late_kernel(level_ref, meta_ref, table_ref, *refs):
    *got_refs, out_ref = refs
    own, other = levels_in(level_ref, meta_ref)
    table = table_ref[own * 3 + other]
    for i, ref in enumerate(got_refs):
        for low, values in pieces(ref):
            out_ref[i, :, low : low + values.shape[1]] = two_part_dot(table, values)


def place_kernel(early, late, early_ref, own_ref, late_ref, filled_ref, out_ref, sems):
    core = core_here()
    run(
        piece_copies(early, 1 - core, 3, early_ref, out_ref, sems.at[0]),
        piece_copies(late, core, 0, own_ref, out_ref, sems.at[1]),
        piece_copies(late, 1 - core, 3, late_ref, out_ref, sems.at[2]),
    )


def member(y, z, core):
    return (y % NY * NZ + z % NZ) * 2 + core


TILES = [
    [member(2 * a + i + core, 2 * b + j + core, core) for i in (0, 1) for j in (0, 1)]
    for core in (0, 1)
    for a in range(NY // 2)
    for b in range(NZ // 2)
]
ALONG_Y = [[[member(2 * a + i, z, core) for a in range(NY // 2)] for i in (0, 1) for z in range(NZ)] for core in (0, 1)]
ALONG_Z = [[[member(y, 2 * b + j, core) for b in range(NZ // 2)] for j in (0, 1) for y in range(NY)] for core in (0, 1)]
LINES = ALONG_Z[0] + ALONG_Y[1]
OTHER_LINES = ALONG_Y[0] + ALONG_Z[1]
VMEM = pl.BlockSpec(memory_space=pltpu.VMEM)
SMEM = pl.BlockSpec(memory_space=pltpu.SMEM)
HBM = pl.BlockSpec(memory_space=pltpu.HBM)
DMA = pltpu.SemaphoreType.DMA


def exchange(values, groups):
    return lax.all_to_all(values, "grp", 0, 0, axis_index_groups=groups, tiled=True)


def f32(*shape):
    return jax.ShapeDtypeStruct(shape, jnp.float32)


def call(kernel, ins, outs, shapes, scratch=(), limit=16, flops=0, moved=0, alias=None):
    return pl.pallas_call(
        kernel,
        in_specs=ins,
        out_specs=outs,
        out_shape=shapes,
        scratch_shapes=scratch,
        compiler_params=pltpu.CompilerParams(vmem_limit_bytes=limit << 20),
        cost_estimate=pl.CostEstimate(flops=flops, bytes_accessed=moved, transcendentals=0),
        input_output_aliases=alias or {},
    )


def shards(grids, first_level, coeffs, slot_map):
    rows = grids[0]
    width = rows.shape[1]
    half = width // 2
    chunk = half // MEMBERS
    slabs = lax.axis_size("slab")
    members = lax.axis_size("grp")
    swap = [(i, i ^ 1) for i in range(members)]
    forth, back = (jnp.asarray(table, jnp.bfloat16) for table in row_tables())

    to_previous = [(i, (i - 1) % slabs) for i in range(slabs)]

    def through_tile(pieces):
        turned = lambda turn: [(tile[i], tile[i ^ turn]) for tile in TILES for i in range(MEMBERS)]
        far = {}
        for turn in (3, 2, 1):
            far[turn] = lax.ppermute(pieces[turn], "grp", turned(turn))
        return [pieces[0], far[1], far[2], far[3]]

    line = call(lead_kernel, [], VMEM, jax.ShapeDtypeStruct((8, LANES), jnp.int32), flops=2*10**9)()
    numbers = call(numbers_kernel, [SMEM, SMEM, VMEM], VMEM, f32(8, LANES))(first_level, coeffs, line)
    entry, plane = call(entry_kernel, [VMEM] * 2, [VMEM] * 2, [f32(ROWS + 8, half), f32(PLANE, width)])(numbers, rows)

    def main_part(*turns):
        return call(
            functools.partial(main_kernel, turns), [SMEM, SMEM] + [VMEM] * 3, [VMEM] * len(turns),
            [f32(SENT, chunk)] * len(turns), flops=10**9,
        )(first_level, coeffs, forth, rows, other)

    def with_next(got, *turns):
        count = len(turns)
        return call(
            functools.partial(next_kernel, turns), [SMEM, SMEM] + [VMEM] * (4 + count), [VMEM] * count,
            [f32(SENT, chunk)] * count, flops=10**8, alias={6 + i: i for i in range(count)},
        )(first_level, coeffs, forth, next_plane, other, other_next, *got)

    next_plane = lax.ppermute(plane, "slab", to_previous)
    other = lax.ppermute(entry, "grp", swap)
    cut = call(cut_kernel, [VMEM], VMEM, f32(PLANE, half))(next_plane)
    other_next = lax.ppermute(cut, "grp", swap)
    sent = main_part(1, 2, 3)
    sent = with_next(sent, 1, 2, 3)
    (stays,) = with_next(main_part(0), 0)
    meta = call(meta_kernel, [VMEM], VMEM, f32(8, LANES))(other)
    got = through_tile([stays, *sent])

    parts = call(add_kernel, [VMEM] * MEMBERS, VMEM, f32(MEMBERS, TABLE, LANES), flops=10**8)(*got)
    for groups in (LINES, OTHER_LINES):
        parts = exchange(parts, groups)
        parts = call(total_kernel, [VMEM], VMEM, f32(MEMBERS, TABLE, LANES), flops=10**8)(parts)
    table = exchange(parts, LINES)
    picked = call(
        pick_kernel, [VMEM] * (MEMBERS + 1), [VMEM] * MEMBERS, [f32(FLAGS, chunk)] * MEMBERS, flops=10**8
    )(table, *got)
    final = through_tile(picked)

    def other_rows(turns):
        return call(
            other_back_kernel, [SMEM] + [VMEM] * (2 + len(turns)), VMEM,
            f32(len(turns), ROWS, chunk), flops=10**9,
        )(first_level, meta, back, *[final[turn] for turn in turns])

    parts = (pltpu.VMEM((4, ROWS, chunk // 2), jnp.float32), DMA((4,)))

    def own_early_rows(turns):
        return call(
            functools.partial(early_kernel, turns), [SMEM] + [VMEM] * 4, HBM, f32(ROWS, width),
            parts, flops=10**9,
        )(first_level, meta, back, *[final[turn] for turn in turns])

    early, late = (0, 3), (2, 1)
    other_early = other_rows(early)
    swapped_early = lax.ppermute(other_early, "grp", swap)
    out = own_early_rows(early)
    other_late = other_rows(late)
    swapped_late = lax.ppermute(other_late, "grp", swap)
    own_late = call(
        late_kernel, [SMEM] + [VMEM] * 4, VMEM, f32(len(late), ROWS, chunk), flops=10**9
    )(first_level, meta, back, *[final[turn] for turn in late])
    out = call(
        functools.partial(place_kernel, early, late), [VMEM] * 3 + [HBM], HBM, f32(ROWS, width),
        (DMA((3, 2)),), alias={3: 0}, flops=10**8,
    )(swapped_early, own_late, swapped_late, out)
    return out[None]


def solution(mesh):
    in_specs = (P("grp", "slab", None), P("grp"), P("grp"), P("grp", "slab"))
    out_specs = P("grp", "slab", None)
    return jax.shard_map(shards, mesh=mesh, in_specs=in_specs, out_specs=out_specs, check_vma=False)
```
